32 devices in a mesh: dp: 1 (over z), ep: 32 (over y, x, core).
Axes of the slice: x: 4, y: 4, z: 1, core: 2. Of those that a mesh axis runs over, the one named last changes fastest.
The devices are a block of a 4x4x8 slice.
Arguments:
- x_in: bfloat16 [8192, 448], P(('dp', 'ep'))
- d_out: bfloat16 [8192, 448], P(('dp', 'ep'))
- idx_a: int32 [8192, 8], P(('dp', 'ep'))
- gate_a: float32 [8192, 8], P(('dp', 'ep'))
- idx_b: int32 [8192, 8], P(('dp', 'ep'))
- gate_b: float32 [8192, 8], P(('dp', 'ep'))
- w1_a: bfloat16 [64, 448, 320], P('ep')
- w3_a: bfloat16 [64, 448, 320], P('ep')
- w2_a: bfloat16 [64, 320, 448], P('ep')
- ws1_a: bfloat16 [448, 2560], replicated
- ws3_a: bfloat16 [448, 2560], replicated
- ws2_a: bfloat16 [2560, 448], replicated
- w1_b: bfloat16 [64, 448, 320], P('ep')
- w3_b: bfloat16 [64, 448, 320], P('ep')
- w2_b: bfloat16 [64, 320, 448], P('ep')
- ws1_b: bfloat16 [448, 2560], replicated
- ws3_b: bfloat16 [448, 2560], replicated
- ws2_b: bfloat16 [2560, 448], replicated
Outputs:
- output 1: bfloat16 [8192, 448], P(('dp', 'ep'))
- output 2: bfloat16 [8192, 448], P(('dp', 'ep'))
- output 3: float32 [64, 448, 320], P(('dp', 'ep'))
- output 4: float32 [64, 448, 320], P(('dp', 'ep'))
- output 5: float32 [64, 320, 448], P(('dp', 'ep'))
- output 6: float32 [64, 448, 320], P(('dp', 'ep'))
- output 7: float32 [64, 448, 320], P(('dp', 'ep'))
- output 8: float32 [64, 320, 448], P(('dp', 'ep'))
- output 9: float32 [8192, 8], P(('dp', 'ep'))
- output 10: float32 [8192, 8], P(('dp', 'ep'))
All inputs are finite; a program needn't handle non-finite values.
Results may differ from the reference program's by a relative error of at most 0.0116113.
Values are sent between devices in bfloat16 or wider.
A program may use at most 768 MiB of HBM per device.

```python
import jax
import jax.numpy as jnp
from jax import lax

D_MODEL = 448
FF_EXPERT = 320
FF_SHARED = 2560
EXPERTS = 64
TOP_K = 8
TOKENS = 256
GROUP_SIZE = 32
REP_COUNT = 8
CAPACITY = 64

PART_TOKENS = GROUP_SIZE * TOKENS
GROUP_ROWS = GROUP_SIZE * CAPACITY


def draw_routing(rng_key):
    fixed_ids = jnp.repeat(jnp.arange(TOP_K, dtype=jnp.int32), REP_COUNT)
    spare_ids = jnp.repeat(jnp.arange(TOP_K, EXPERTS, dtype=jnp.int32), REP_COUNT)

    def one_device(dev_key):
        sub_keys = jax.random.split(dev_key, 4)
        picked = jax.random.permutation(sub_keys[0], spare_ids)[: TOKENS - TOP_K * REP_COUNT]
        base_ids = jax.random.permutation(sub_keys[1], jnp.concatenate([fixed_ids, picked]))
        shift_by = jax.random.randint(sub_keys[2], (), 0, EXPERTS, dtype=jnp.int32)
        turn_by = jax.random.randint(sub_keys[3], (TOKENS, 1), 0, TOP_K, dtype=jnp.int32)
        offsets = (jnp.arange(TOP_K, dtype=jnp.int32)[None, :] + turn_by) % TOP_K
        return (base_ids[:, None] + offsets + shift_by) % EXPERTS

    dev_keys = jax.random.split(rng_key, GROUP_SIZE)
    return jax.vmap(one_device)(dev_keys).reshape(PART_TOKENS, TOP_K)


def normal_bf16(rng_key, out_shape, scale):
    return (jax.random.normal(rng_key, out_shape, jnp.float32) * scale).astype(jnp.bfloat16)


def layer_weights(weight_keys, key_start):
    return (
        normal_bf16(weight_keys[key_start], (EXPERTS, D_MODEL, FF_EXPERT), D_MODEL ** -0.5),
        normal_bf16(weight_keys[key_start + 1], (EXPERTS, D_MODEL, FF_EXPERT), D_MODEL ** -0.5),
        normal_bf16(weight_keys[key_start + 2], (EXPERTS, FF_EXPERT, D_MODEL), FF_EXPERT ** -0.5),
        normal_bf16(weight_keys[key_start + 3], (D_MODEL, FF_SHARED), D_MODEL ** -0.5),
        normal_bf16(weight_keys[key_start + 4], (D_MODEL, FF_SHARED), D_MODEL ** -0.5),
        normal_bf16(weight_keys[key_start + 5], (FF_SHARED, D_MODEL), FF_SHARED ** -0.5),
    )


def setup_inputs(seed: int = 0, part: int = 0) -> dict:
    part_keys = jax.random.split(jax.random.fold_in(jax.random.key(seed), part), 6)
    weight_keys = jax.random.split(jax.random.key(seed + 1), 12)
    gate_scale = TOP_K ** -0.5
    w1_a, w3_a, w2_a, ws1_a, ws3_a, ws2_a = layer_weights(weight_keys, 0)
    w1_b, w3_b, w2_b, ws1_b, ws3_b, ws2_b = layer_weights(weight_keys, 6)
    return {
        'x_in': normal_bf16(part_keys[0], (PART_TOKENS, D_MODEL), 1.0),
        'd_out': normal_bf16(part_keys[1], (PART_TOKENS, D_MODEL), 1.0),
        'idx_a': draw_routing(part_keys[2]),
        'gate_a': jax.random.uniform(part_keys[3], (PART_TOKENS, TOP_K), jnp.float32, 0.5, 1.5) * gate_scale,
        'idx_b': draw_routing(part_keys[4]),
        'gate_b': jax.random.uniform(part_keys[5], (PART_TOKENS, TOP_K), jnp.float32, 0.5, 1.5) * gate_scale,
        'w1_a': w1_a, 'w3_a': w3_a, 'w2_a': w2_a,
        'ws1_a': ws1_a, 'ws3_a': ws3_a, 'ws2_a': ws2_a,
        'w1_b': w1_b, 'w3_b': w3_b, 'w2_b': w2_b,
        'ws1_b': ws1_b, 'ws3_b': ws3_b, 'ws2_b': ws2_b,
    }


def route_tables(expert_ids):
    flat_ids = expert_ids.reshape(-1)
    pair_count = flat_ids.shape[0]
    pair_order = jnp.argsort(flat_ids, stable=True)
    expert_count = jax.ops.segment_sum(jnp.ones_like(flat_ids), flat_ids, num_segments=EXPERTS)
    expert_start = jnp.cumsum(expert_count) - expert_count
    position = flat_ids * GROUP_ROWS + jnp.argsort(pair_order) - expert_start[flat_ids]
    slot_index = jnp.arange(GROUP_ROWS)
    src_pair = pair_order[jnp.minimum(expert_start[:, None] + slot_index[None, :], pair_count - 1)]
    slot_used = slot_index[None, :] < expert_count[:, None]
    return src_pair, slot_used, position


def swiglu_hidden(rows, w_gate, w_up):
    pre_gate = jnp.dot(rows, w_gate, preferred_element_type=jnp.float32)
    pre_up = jnp.dot(rows, w_up, preferred_element_type=jnp.float32)
    return pre_gate, pre_up, (jax.nn.silu(pre_gate) * pre_up).astype(jnp.bfloat16)


def swiglu_grads(pre_gate, pre_up, d_hidden):
    sigma = jax.nn.sigmoid(pre_gate)
    d_gate = d_hidden * pre_up * sigma * (1.0 + pre_gate * (1.0 - sigma))
    d_up = d_hidden * pre_gate * sigma
    return d_gate.astype(jnp.bfloat16), d_up.astype(jnp.bfloat16)


def layer_forward(x_rows, expert_ids, gates, w_gate, w_up, w_down, s_gate, s_up, s_down):
    src_pair, slot_used, position = route_tables(expert_ids)
    sent = jnp.where(slot_used[:, :, None], x_rows[src_pair // TOP_K], 0)

    def one_expert(operands):
        rows, gate_w, up_w, down_w = operands
        hidden = swiglu_hidden(rows, gate_w, up_w)[2]
        return jnp.dot(hidden, down_w, preferred_element_type=jnp.float32).astype(jnp.bfloat16)

    expert_out = lax.map(one_expert, (sent, w_gate, w_up, w_down))
    per_pair = expert_out.reshape(-1, D_MODEL)[position].reshape(PART_TOKENS, TOP_K, D_MODEL)
    shared = jnp.dot(swiglu_hidden(x_rows, s_gate, s_up)[2], s_down, preferred_element_type=jnp.float32)
    mixed = x_rows.astype(jnp.float32) + shared + jnp.sum(gates[:, :, None] * per_pair.astype(jnp.float32), axis=1)
    return mixed.astype(jnp.bfloat16)


def layer_backward(x_rows, d_next, expert_ids, gates, w_gate, w_up, w_down, s_gate, s_up, s_down):
    src_pair, slot_used, position = route_tables(expert_ids)
    src_token = src_pair // TOP_K
    sent = jnp.where(slot_used[:, :, None], x_rows[src_token], 0)
    sent_dy = jnp.where(slot_used[:, :, None], d_next[src_token], 0)
    sent_gate = jnp.where(slot_used, gates.reshape(-1)[src_pair], 0.0)

    def one_expert(operands):
        rows, dy_part, gate_part, gate_w, up_w, down_w = operands
        pre_gate, pre_up, hidden = swiglu_hidden(rows, gate_w, up_w)
        projected = jnp.dot(dy_part, down_w.T, preferred_element_type=jnp.float32)
        gate_grad = jnp.sum(hidden.astype(jnp.float32) * projected, axis=1)
        scaled = (gate_part[:, None] * dy_part.astype(jnp.float32)).astype(jnp.bfloat16)
        dw_down = jnp.dot(hidden.T, scaled, preferred_element_type=jnp.float32)
        da_gate, da_up = swiglu_grads(pre_gate, pre_up, gate_part[:, None] * projected)
        dw_gate = jnp.dot(rows.T, da_gate, preferred_element_type=jnp.float32)
        dw_up = jnp.dot(rows.T, da_up, preferred_element_type=jnp.float32)
        d_rows = (jnp.dot(da_gate, gate_w.T, preferred_element_type=jnp.float32)
                  + jnp.dot(da_up, up_w.T, preferred_element_type=jnp.float32)).astype(jnp.bfloat16)
        return dw_gate, dw_up, dw_down, d_rows, gate_grad

    dw_gate, dw_up, dw_down, d_sent, gate_grad = lax.map(
        one_expert, (sent, sent_dy, sent_gate, w_gate, w_up, w_down))
    du_pair = d_sent.reshape(-1, D_MODEL)[position].reshape(PART_TOKENS, TOP_K, D_MODEL)
    d_gates = gate_grad.reshape(-1)[position].reshape(PART_TOKENS, TOP_K)
    s_pre = swiglu_hidden(x_rows, s_gate, s_up)
    s_projected = jnp.dot(d_next, s_down.T, preferred_element_type=jnp.float32)
    ds_gate, ds_up = swiglu_grads(s_pre[0], s_pre[1], s_projected)
    shared_dx = (jnp.dot(ds_gate, s_gate.T, preferred_element_type=jnp.float32)
                 + jnp.dot(ds_up, s_up.T, preferred_element_type=jnp.float32))
    d_x = d_next.astype(jnp.float32) + shared_dx + jnp.sum(du_pair.astype(jnp.float32), axis=1)
    return d_x.astype(jnp.bfloat16), dw_gate, dw_up, dw_down, d_gates


def reference(x_in, d_out, idx_a, gate_a, idx_b, gate_b,
              w1_a, w3_a, w2_a, ws1_a, ws3_a, ws2_a,
              w1_b, w3_b, w2_b, ws1_b, ws3_b, ws2_b):
    x_mid = layer_forward(x_in, idx_a, gate_a, w1_a, w3_a, w2_a, ws1_a, ws3_a, ws2_a)
    x_last = layer_forward(x_mid, idx_b, gate_b, w1_b, w3_b, w2_b, ws1_b, ws3_b, ws2_b)
    d_mid, dw1_b, dw3_b, dw2_b, dgate_b = layer_backward(
        x_mid, d_out, idx_b, gate_b, w1_b, w3_b, w2_b, ws1_b, ws3_b, ws2_b)
    d_first, dw1_a, dw3_a, dw2_a, dgate_a = layer_backward(
        x_in, d_mid, idx_a, gate_a, w1_a, w3_a, w2_a, ws1_a, ws3_a, ws2_a)
    return (x_last, d_first, dw1_a, dw3_a, dw2_a, dw1_b, dw3_b, dw2_b, dgate_a, dgate_b)
```

```python
import functools
import math

import jax
import jax.numpy as jnp
from jax import lax
from jax.experimental import pallas as pl
from jax.experimental.pallas import tpu as pltpu
from jax.sharding import PartitionSpec as P

MESH = pl.DeviceIdType.MESH
F32, BF16 = jnp.float32, jnp.bfloat16
NT = (((1,), (1,)), ((), ()))
VMEM_LIMIT = 60 * 2 ** 20


def dev(i):
    return {'ep': i}


class Torus:
    def __init__(self, n):
        self.nx = math.isqrt(n // 2)
        self.ny = n // 2 // self.nx
        self.me = lax.axis_index('ep')
        self.c = lax.rem(self.me, 2)
        chip = self.me // 2
        self.x, self.y = lax.rem(chip, self.nx), chip // self.nx

    def at(self, dx, dy, c=None):
        x = lax.rem(self.x + dx + self.nx, self.nx)
        y = lax.rem(self.y + dy + self.ny, self.ny)
        return (y * self.nx + x) * 2 + (self.c if c is None else c)


def barrier_all(n):
    me = lax.axis_index('ep')
    b = pltpu.get_barrier_semaphore()

    def body(k, _):
        pl.semaphore_signal(b, inc=1, device_id=dev(lax.rem(me + k, n)), device_id_type=MESH)
        return 0

    lax.fori_loop(1, n, body, 0)
    pl.semaphore_wait(b, n - 1)


def remote(src, dst, ssem, rsem, to):
    return pltpu.make_async_remote_copy(src_ref=src, dst_ref=dst, send_sem=ssem, recv_sem=rsem,
                                        device_id=dev(to), device_id_type=MESH)


class Gather:
    def __init__(self, torus, out, ssem, rsem, rows):
        self.t, self.out, self.ssem, self.rsem = torus, out, ssem, rsem
        self.half, self.quarter = rows // 2, rows // 4
        self.count, self.sent, self.sibling, self.m = 0, [], [], {}

    def ref(self, off, r0, nr, core=None):
        return self.out.at[self.t.at(off[0], off[1], core), pl.ds(r0, nr), :]

    def move(self, off, r0, nr, to):
        i = self.count
        self.count += 1
        ref = self.ref(off, r0, nr)
        cp = remote(ref, ref, self.ssem.at[i], self.rsem.at[i], self.t.at(*to))
        cp.start()
        self.sent.append(cp)
        return i, nr

    def wait(self, off, r0, mv):
        i, nr = mv
        ref = self.ref(off, r0, nr)
        remote(ref, ref, self.ssem.at[i], self.rsem.at[i], self.t.at(1, 0)).wait_recv()

    def to_sibling(self, off, r0, nr):
        i = self.count
        self.count += 1
        ref = self.ref(off, r0, nr)
        cp = remote(ref, ref, self.ssem.at[i], self.rsem.at[i], self.t.at(0, 0, 1 - self.t.c))
        cp.start()
        self.sent.append(cp)
        self.sibling.append((off, r0, nr, i))

    @staticmethod
    def ax(h, d, e=0):
        return (d, e) if h == 0 else (e, d)

    def start(self):
        ax, m = self.ax, self.m
        for h in (0, 1):
            for d in (1, -1):
                m[h, 1, d] = self.move((0, 0), h * self.half, self.half, ax(h, d))
        for h in (0, 1):
            for d in (1, -1):
                m[h, 2, 0, d] = self.move((0, 0), h * self.half, self.half, ax(h, 0, d))
        self.to_sibling((0, 0), 0, 2 * self.half)

    def run(self):
        ax, m, half, q = self.ax, self.m, self.half, self.quarter
        for h in (0, 1):
            for k, d in enumerate((1, -1)):
                self.wait(ax(h, -d), h * half, m[h, 1, d])
                m[h, 1, d, 'f'] = self.move(ax(h, -d), h * half + k * q, q, ax(h, d))
                for e in (1, -1):
                    m[h, 2, -d, e] = self.move(ax(h, -d), h * half, half, ax(h, 0, e))
                self.to_sibling(ax(h, -d), h * half, half)
        for h in (0, 1):
            for k, e in enumerate((1, -1)):
                self.wait(ax(h, 0, -e), h * half, m[h, 2, 0, e])
                m[h, 2, 0, e, 'f'] = self.move(ax(h, 0, -e), h * half + k * q, q, ax(h, 0, e))
                self.to_sibling(ax(h, 0, -e), h * half, half)
        for h in (0, 1):
            for k, d in enumerate((1, -1)):
                self.wait(ax(h, -2 * d), h * half + k * q, m[h, 1, d, 'f'])
            for e in (1, -1):
                m[h, 2, 2, e] = self.move(ax(h, 2), h * half, half, ax(h, 0, e))
            self.to_sibling(ax(h, 2), h * half, half)
        for b in (-1, 1, 2):
            for h in (0, 1):
                for k, e in enumerate((1, -1)):
                    self.wait(ax(h, b, -e), h * half, m[h, 2, b, e])
                    m[h, 2, b, e, 'f'] = self.move(ax(h, b, -e), h * half + k * q, q, ax(h, 0, e))
                    self.to_sibling(ax(h, b, -e), h * half, half)
        for b in (0, -1, 1, 2):
            for h in (0, 1):
                for k, e in enumerate((1, -1)):
                    self.wait(ax(h, b, -2 * e), h * half + k * q, m[h, 2, b, e, 'f'])
                self.to_sibling(ax(h, b, 2), h * half, half)

    def finish(self):
        for off, r0, nr, i in self.sibling:
            ref = self.ref(off, r0, nr, 1 - self.t.c)
            remote(ref, ref, self.ssem.at[i], self.rsem.at[i], self.t.at(1, 0)).wait_recv()
        for cp in self.sent:
            cp.wait_send()


GATHER_SEMS = 80


def gather_kernel(n, x_ref, out_ref, ssem, rsem, lsem):
    t = Torus(n)
    barrier_all(n)
    own = pltpu.make_async_copy(x_ref, out_ref.at[t.me], lsem.at[0])
    own.start()
    own.wait()
    g = Gather(t, out_ref, ssem, rsem, x_ref.shape[0])
    g.start()
    g.run()
    g.finish()


def all_gather(x, n, cid):
    return pl.pallas_call(
        functools.partial(gather_kernel, n),
        out_shape=jax.ShapeDtypeStruct((n,) + x.shape, x.dtype),
        in_specs=[pl.BlockSpec(memory_space=pl.ANY)],
        out_specs=pl.BlockSpec(memory_space=pl.ANY),
        scratch_shapes=[pltpu.SemaphoreType.DMA((GATHER_SEMS,)), pltpu.SemaphoreType.DMA((GATHER_SEMS,)),
                        pltpu.SemaphoreType.DMA((1,))],
        compiler_params=pltpu.CompilerParams(collective_id=cid, has_side_effects=True),
    )(x)


def exchange_kernel(n, *refs):
    count = (len(refs) - 3) // 2
    ins, outs, (ssem, rsem, lsem) = refs[:count], refs[count:2 * count], refs[2 * count:]
    me = lax.axis_index('ep')
    barrier_all(n)
    own = [pltpu.make_async_copy(a.at[me], b.at[me], lsem.at[i]) for i, (a, b) in enumerate(zip(ins, outs))]
    for cp in own:
        cp.start()

    def sends(k):
        to = lax.rem(me + k, n)
        return [remote(a.at[to], b.at[me], ssem.at[i, k], rsem.at[i, k], to)
                for i, (a, b) in enumerate(zip(ins, outs))]

    def arrivals(k):
        fr = lax.rem(me - k + n, n)
        return [remote(a.at[fr], b.at[fr], ssem.at[i, k], rsem.at[i, k], fr)
                for i, (a, b) in enumerate(zip(ins, outs))]

    def start(k, _):
        for cp in sends(k):
            cp.start()
        return 0

    def wait(k, _):
        for cp in arrivals(k):
            cp.wait_recv()
        for cp in sends(k):
            cp.wait_send()
        return 0

    lax.fori_loop(1, n, start, 0)
    lax.fori_loop(1, n, wait, 0)
    for cp in own:
        cp.wait()


def exchange(arrays, n, cid):
    count = len(arrays)
    return pl.pallas_call(
        functools.partial(exchange_kernel, n),
        out_shape=[jax.ShapeDtypeStruct(a.shape, a.dtype) for a in arrays],
        in_specs=[pl.BlockSpec(memory_space=pl.ANY)] * count,
        out_specs=[pl.BlockSpec(memory_space=pl.ANY)] * count,
        scratch_shapes=[pltpu.SemaphoreType.DMA((count, n)), pltpu.SemaphoreType.DMA((count, n)),
                        pltpu.SemaphoreType.DMA((count,))],
        compiler_params=pltpu.CompilerParams(collective_id=cid, has_side_effects=True),
    )(*arrays)


def mm(a, b):
    return jnp.dot(a, b, preferred_element_type=F32)


def mm_nt(a, b):
    return lax.dot_general(a, b, NT, preferred_element_type=F32)


def slots_of(gates):
    tokens = gates.shape[1]
    before = (lax.broadcasted_iota(jnp.int32, (tokens, tokens), 0)
              < lax.broadcasted_iota(jnp.int32, (tokens, tokens), 1))
    member = gates > 0.0
    count = mm(jnp.where(member, 1.0, 0.0).astype(BF16), jnp.where(before, 1.0, 0.0).astype(BF16))
    return jnp.where(member, count, -1.0)


def pick(slot_rows, capacity):
    tokens = slot_rows[0].shape[1]
    want = lax.broadcasted_iota(jnp.int32, (capacity, tokens), 0).astype(F32)
    return jnp.concatenate([jnp.where(s == want, 1.0, 0.0) for s in slot_rows], axis=0)


def split3(v):
    a = v.astype(BF16).astype(F32)
    r = v - a
    b = r.astype(BF16).astype(F32)
    return a, b, r - b


def swap_halves(first, second):
    low = lax.broadcasted_iota(jnp.int32, first.shape, 1) < first.shape[1] // 2
    return jnp.where(low, first, second), jnp.where(low, second, first)


def hidden_of(a13):
    f = a13.shape[0] // 2
    a1, a3 = a13[:f], a13[f:]
    sigma = jax.nn.sigmoid(a1)
    return a1, a3, sigma, (a1 * sigma * a3).astype(BF16)


def pair_rows(block, p, slots, row, capacity, extra=None):
    out = []
    for s in (2 * p, 2 * p + 1):
        hot = pick([slots[8 * s + row:8 * s + row + 1], slots[8 * s + row + 1:8 * s + row + 2]], capacity).astype(BF16)
        lhs = block[s] if extra is None else jnp.concatenate([block[s], extra[s]], axis=0)
        out.append(mm_nt(lhs, hot))
    return swap_halves(*out)


def forward_kernel(row, capacity, keep, x_ref, g_ref, w13t_ref, w2t_ref, *outs):
    o_ref = outs[0]
    sources = x_ref.shape[0]
    slots = slots_of(g_ref[...].reshape(sources * 8, -1))
    pairs = [pair_rows(x_ref, p, slots, row, capacity) for p in range(sources // 2)]
    o = []
    for e in (0, 1):
        rows = jnp.concatenate([pr[e].astype(BF16) for pr in pairs], axis=1)
        if keep:
            outs[1][e] = rows
        hidden = hidden_of(mm(w13t_ref[e], rows))[3]
        o.append(mm(w2t_ref[e], hidden))
    width = 2 * capacity
    for p in range(sources // 2):
        a, b = swap_halves(o[0][:, p * width:(p + 1) * width], o[1][:, p * width:(p + 1) * width])
        o_ref[2 * p] = a.astype(BF16)
        o_ref[2 * p + 1] = b.astype(BF16)


def backward_kernel(row, capacity, kept, x_ref, dy_ref, g_ref, w13t_ref, w13_ref, w2_ref,
                    dw1_ref, dw3_ref, dw2_ref, du_ref, gg_ref, acc13, acc2):
    sources = dy_ref.shape[0]
    step = pl.program_id(0)

    @pl.when(step == 0)
    def _():
        acc13[...] = jnp.zeros_like(acc13)
        acc2[...] = jnp.zeros_like(acc2)

    d = dy_ref.shape[1]
    width = 2 * capacity
    slots = slots_of(g_ref[...].reshape(sources * 8, -1))
    extra = []
    for s in range(sources):
        parts = split3(g_ref[s])
        extra.append(jnp.concatenate(list(parts) + [jnp.zeros_like(parts[0])], axis=0).astype(BF16))
    if not kept:
        xp = [pair_rows(x_ref, p, slots, row, capacity) for p in range(sources // 2)]
    dyp, gp = [], []
    for p in range(sources // 2):
        raw = []
        for s in (2 * p, 2 * p + 1):
            hot = pick([slots[8 * s + row:8 * s + row + 1], slots[8 * s + row + 1:8 * s + row + 2]],
                       capacity).astype(BF16)
            raw.append(mm_nt(jnp.concatenate([dy_ref[s], extra[s]], axis=0), hot))
        dyp.append(swap_halves(raw[0][:d], raw[1][:d]))
        gates = []
        for r in raw:
            first = r[d + row:d + row + 1] + r[d + 8 + row:d + 9 + row] + r[d + 16 + row:d + 17 + row]
            second = r[d + row + 1:d + row + 2] + r[d + 9 + row:d + 10 + row] + r[d + 17 + row:d + 18 + row]
            low = lax.broadcasted_iota(jnp.int32, first.shape, 1) < capacity
            gates.append(jnp.where(low, first, second))
        gp.append(swap_halves(*gates))
    du, gg = [], []
    for e in (0, 1):
        rows = x_ref[e] if kept else jnp.concatenate([pr[e].astype(BF16) for pr in xp], axis=1)
        dy = jnp.concatenate([pr[e] for pr in dyp], axis=1)
        gate = jnp.concatenate([pr[e] for pr in gp], axis=1)
        a1, a3, sigma, hidden = hidden_of(mm(w13t_ref[e], rows))
        p32 = mm(w2_ref[e], dy.astype(BF16))
        gg.append(jnp.sum(hidden.astype(F32) * p32, axis=0, keepdims=True))
        scaled = (gate * dy).astype(BF16)
        acc2[e] += mm_nt(hidden, scaled)
        q = gate * p32
        da1 = (q * a3 * sigma * (1.0 + a1 * (1.0 - sigma))).astype(BF16)
        da3 = (q * a1 * sigma).astype(BF16)
        da = jnp.concatenate([da1, da3], axis=0)
        acc13[e] += mm_nt(rows, da)
        du.append(mm(w13_ref[e], da))
    for p in range(sources // 2):
        at = slice(p * width, (p + 1) * width)
        for ref, v in ((du_ref, du), (gg_ref, gg)):
            a, b = swap_halves(v[0][:, at], v[1][:, at])
            ref[2 * p] = jnp.broadcast_to(a, ref.shape[1:]).astype(ref.dtype)
            ref[2 * p + 1] = jnp.broadcast_to(b, ref.shape[1:]).astype(ref.dtype)

    @pl.when(step == pl.num_programs(0) - 1)
    def _():
        f = dw1_ref.shape[2]
        for e in (0, 1):
            dw1_ref[e] = acc13[e, :, :f]
            dw3_ref[e] = acc13[e, :, f:]
            dw2_ref[e] = acc2[e]


SOURCES = 4


def whole(a):
    return pl.BlockSpec(a.shape, lambda i: (0,) * a.ndim)


def experts_forward(xg, gr, w13t, w2t, row, capacity, keep):
    n, d, tokens = xg.shape
    lanes = SOURCES * capacity
    out_shape = [jax.ShapeDtypeStruct((n, d, 2 * capacity), BF16)]
    out_specs = [pl.BlockSpec((SOURCES, d, 2 * capacity), lambda i: (i, 0, 0))]
    if keep:
        out_shape.append(jax.ShapeDtypeStruct((2, d, n * capacity), BF16))
        out_specs.append(pl.BlockSpec((2, d, lanes), lambda i: (0, 0, i)))
    return pl.pallas_call(
        functools.partial(forward_kernel, row, capacity, keep),
        grid=(n // SOURCES,),
        out_shape=out_shape, out_specs=out_specs,
        in_specs=[pl.BlockSpec((SOURCES, d, tokens), lambda i: (i, 0, 0)),
                  pl.BlockSpec((SOURCES, 8, tokens), lambda i: (i, 0, 0)), whole(w13t), whole(w2t)],
        compiler_params=pltpu.CompilerParams(vmem_limit_bytes=VMEM_LIMIT),
    )(xg, gr, w13t, w2t)


def experts_backward(x, dyg, gr, w13t, w13, w2, row, capacity, kept):
    n, d, tokens = dyg.shape
    lanes = SOURCES * capacity
    f = w2.shape[1]
    grouped = lambda i: (i, 0, 0)
    x_spec = (pl.BlockSpec((2, d, lanes), lambda i: (0, 0, i)) if kept
              else pl.BlockSpec((SOURCES, d, tokens), grouped))
    grads = [jax.ShapeDtypeStruct((2, d, f), F32)] * 2 + [jax.ShapeDtypeStruct((2, f, d), F32)]
    return pl.pallas_call(
        functools.partial(backward_kernel, row, capacity, kept),
        grid=(n // SOURCES,),
        out_shape=grads + [jax.ShapeDtypeStruct((n, d, 2 * capacity), BF16),
                           jax.ShapeDtypeStruct((n, 8, 2 * capacity), F32)],
        out_specs=[whole(g) for g in grads] + [pl.BlockSpec((SOURCES, d, 2 * capacity), grouped),
                                               pl.BlockSpec((SOURCES, 8, 2 * capacity), grouped)],
        in_specs=[x_spec, pl.BlockSpec((SOURCES, d, tokens), grouped),
                  pl.BlockSpec((SOURCES, 8, tokens), grouped), whole(w13t), whole(w13), whole(w2)],
        scratch_shapes=[pltpu.VMEM((2, d, 2 * f), F32), pltpu.VMEM((2, f, d), F32)],
        compiler_params=pltpu.CompilerParams(vmem_limit_bytes=VMEM_LIMIT),
    )(x, dyg, gr, w13t, w13, w2)


def combine_forward_kernel(row, capacity, o_ref, g_ref, y_ref):
    step = pl.program_id(0)
    senders = o_ref.shape[0]
    slots = slots_of(g_ref[...].reshape(senders * 8, -1))

    @pl.when(step == 0)
    def _():
        y_ref[...] = jnp.zeros_like(y_ref)

    acc = y_ref[...]
    for p in range(senders // 2):
        ks = (2 * p, 2 * p + 1)
        lhs = jnp.concatenate([o_ref[k] for k in ks], axis=1)
        order = [8 * k + row + e for k in ks for e in (0, 1)]
        hot = pick([slots[r:r + 1] for r in order], capacity)
        gates = [g_ref[k, row + e:row + e + 1] for k in ks for e in (0, 1)]
        parts = [split3(g) for g in gates]
        for i in range(3):
            part = jnp.concatenate([jnp.broadcast_to(q[i], (capacity,) + q[i].shape[1:]) for q in parts], axis=0)
            acc = acc + mm(lhs, (hot * part).astype(BF16))
    y_ref[...] = acc


def combine_backward_kernel(row, capacity, du_ref, gg_ref, g_ref, y_ref, dg_ref):
    step = pl.program_id(0)
    senders, d = du_ref.shape[0], du_ref.shape[1]
    slots = slots_of(g_ref[...].reshape(senders * 8, -1))

    @pl.when(step == 0)
    def _():
        y_ref[...] = jnp.zeros_like(y_ref)

    acc = y_ref[...]
    dgs = []
    for p in range(senders // 2):
        ks = (2 * p, 2 * p + 1)
        order = [8 * k + row + e for k in ks for e in (0, 1)]
        hot = pick([slots[r:r + 1] for r in order], capacity).astype(BF16)
        gg = jnp.concatenate([gg_ref[k] for k in ks], axis=1)
        shape = gg.shape
        own = (lax.broadcasted_iota(jnp.int32, shape, 1) // capacity) == lax.broadcasted_iota(jnp.int32, shape, 0)
        parts = split3(jnp.where(own, gg, 0.0))
        small = jnp.concatenate(list(parts) + [jnp.zeros_like(parts[0])], axis=0).astype(BF16)
        lhs = jnp.concatenate([jnp.concatenate([du_ref[k] for k in ks], axis=1), small], axis=0)
        res = mm(lhs, hot)
        acc = acc + res[:d]
        dgs.append((res[d:d + 8] + res[d + 8:d + 16] + res[d + 16:d + 24])[:4])
    y_ref[...] = acc
    dg_ref[...] = jnp.concatenate(dgs, axis=0)


SENDERS = 8


def combine_forward(o, g_own, row, capacity):
    n, d, _ = o.shape
    tokens = g_own.shape[2]
    return pl.pallas_call(
        functools.partial(combine_forward_kernel, row, capacity),
        grid=(n // SENDERS,),
        out_shape=jax.ShapeDtypeStruct((d, tokens), F32),
        out_specs=pl.BlockSpec((d, tokens), lambda i: (0, 0)),
        in_specs=[pl.BlockSpec((SENDERS, d, 2 * capacity), lambda i: (i, 0, 0)),
                  pl.BlockSpec((SENDERS, 8, tokens), lambda i: (i, 0, 0))],
        compiler_params=pltpu.CompilerParams(vmem_limit_bytes=VMEM_LIMIT),
    )(o, g_own)


def combine_backward(du, gg, g_own, row, capacity):
    n, d, _ = du.shape
    tokens = g_own.shape[2]
    return pl.pallas_call(
        functools.partial(combine_backward_kernel, row, capacity),
        grid=(n // SENDERS,),
        out_shape=[jax.ShapeDtypeStruct((d, tokens), F32), jax.ShapeDtypeStruct((2 * n, tokens), F32)],
        out_specs=[pl.BlockSpec((d, tokens), lambda i: (0, 0)),
                   pl.BlockSpec((2 * SENDERS, tokens), lambda i: (i, 0))],
        in_specs=[pl.BlockSpec((SENDERS, d, 2 * capacity), lambda i: (i, 0, 0)),
                  pl.BlockSpec((SENDERS, 8, 2 * capacity), lambda i: (i, 0, 0)),
                  pl.BlockSpec((SENDERS, 8, tokens), lambda i: (i, 0, 0))],
        compiler_params=pltpu.CompilerParams(vmem_limit_bytes=VMEM_LIMIT),
    )(du, gg, g_own)


def swiglu_grads(pre_gate, pre_up, d_hidden):
    sigma = jax.nn.sigmoid(pre_gate)
    d_gate = d_hidden * pre_up * sigma * (1.0 + pre_gate * (1.0 - sigma))
    d_up = d_hidden * pre_gate * sigma
    return d_gate.astype(BF16), d_up.astype(BF16)


def shared_hidden(rows, s_gate, s_up):
    pre_gate, pre_up = mm(rows, s_gate), mm(rows, s_up)
    return pre_gate, pre_up, (jax.nn.silu(pre_gate) * pre_up).astype(BF16)


def shared_input_grad(x_rows, d_next, s_gate, s_up, s_down):
    pre = shared_hidden(x_rows, s_gate, s_up)
    ds_gate, ds_up = swiglu_grads(pre[0], pre[1], mm_nt(d_next, s_down))
    return mm_nt(ds_gate, s_gate) + mm_nt(ds_up, s_up)


def gate_table(idx, gate, n_experts):
    ids = jnp.arange(n_experts, dtype=idx.dtype)[:, None, None]
    return jnp.sum(jnp.where(idx.T[None] == ids, gate.T[None], 0.0), axis=1)


def pair_gates(dg, idx):
    ids = jnp.arange(dg.shape[0], dtype=idx.dtype)[:, None, None]
    return jnp.sum(jnp.where(idx.T[None] == ids, dg[:, None, :], 0.0), axis=0).T


def solution(mesh):
    n = mesh.shape['ep']
    token_spec = P(('dp', 'ep'), None)
    expert_spec = P('ep', None, None)
    shared_spec = P(None, None)
    grad_spec = P(('dp', 'ep'), None, None)
    layer_specs = (expert_spec,) * 3 + (shared_spec,) * 3

    def device_step(x_in, d_out, idx_a, gate_a, idx_b, gate_b,
                    w1_a, w3_a, w2_a, ws1_a, ws3_a, ws2_a,
                    w1_b, w3_b, w2_b, ws1_b, ws3_b, ws2_b):
        tokens, top_k = idx_a.shape
        n_experts = w1_a.shape[0] * n
        capacity = top_k * ((2 * tokens + n_experts - 1) // n_experts)

        def weights(w1, w3, w2):
            w13 = jnp.concatenate([w1, w3], axis=2)
            return jnp.swapaxes(w13, 1, 2), w13, w2, jnp.swapaxes(w2, 1, 2)

        w13t_a, w13_a, w2n_a, w2t_a = weights(w1_a, w3_a, w2_a)
        w13t_b, w13_b, w2n_b, w2t_b = weights(w1_b, w3_b, w2_b)

        odd = lax.rem(lax.axis_index('ep'), 2) == 1
        tables = [gate_table(i, g, n_experts).reshape(n, 2, tokens) for i, g in ((idx_a, gate_a), (idx_b, gate_b))]
        tables = [jnp.where(odd, t[:, ::-1], t) for t in tables]
        g_own = jnp.concatenate(tables + [jnp.zeros((n, 4, tokens), F32)], axis=1)

        (g_recv,) = exchange([g_own], n, 0)
        xg = all_gather(x_in.T, n, 1)
        (o_a,) = experts_forward(xg, g_recv, w13t_a, w2t_a, 0, capacity, False)
        (ret_a,) = exchange([o_a], n, 2)
        mixed_a = combine_forward(ret_a, g_own, 0, capacity)
        shared_a = mm(shared_hidden(x_in, ws1_a, ws3_a)[2], ws2_a)
        x_mid = (x_in.astype(F32) + shared_a + mixed_a.T).astype(BF16)

        x1g = all_gather(x_mid.T, n, 3)
        o_b, rows_b = experts_forward(x1g, g_recv, w13t_b, w2t_b, 2, capacity, True)
        (ret_b,) = exchange([o_b], n, 4)
        mixed_b = combine_forward(ret_b, g_own, 2, capacity)
        shared_b = mm(shared_hidden(x_mid, ws1_b, ws3_b)[2], ws2_b)
        x_last = (x_mid.astype(F32) + shared_b + mixed_b.T).astype(BF16)

        def unswap(dg):
            dg = dg.reshape(n, 2, tokens)
            return jnp.where(odd, dg[:, ::-1], dg).reshape(2 * n, tokens)

        dyg = all_gather(d_out.T, n, 5)
        dw1_b, dw3_b, dw2_b, du_b, gg_b = experts_backward(rows_b, dyg, g_recv, w13t_b, w13_b, w2n_b, 2, capacity, True)
        du_ret_b, gg_ret_b = exchange([du_b, gg_b], n, 6)
        dx_b, dg_b = combine_backward(du_ret_b, gg_ret_b, g_own, 2, capacity)
        shared_dx = shared_input_grad(x_mid, d_out, ws1_b, ws3_b, ws2_b)
        d_mid = (d_out.astype(F32) + shared_dx + dx_b.T).astype(BF16)

        xg2 = all_gather(lax.optimization_barrier((x_in.T, d_mid))[0], n, 7)
        dyg2 = all_gather(d_mid.T, n, 8)
        dw1_a, dw3_a, dw2_a, du_a, gg_a = experts_backward(xg2, dyg2, g_recv, w13t_a, w13_a, w2n_a, 0, capacity, False)
        du_ret_a, gg_ret_a = exchange([du_a, gg_a], n, 9)
        dx_a, dg_a = combine_backward(du_ret_a, gg_ret_a, g_own, 0, capacity)
        shared_dx = shared_input_grad(x_in, d_mid, ws1_a, ws3_a, ws2_a)
        d_first = (d_mid.astype(F32) + shared_dx + dx_a.T).astype(BF16)
        return (x_last, d_first, dw1_a, dw3_a, dw2_a, dw1_b, dw3_b, dw2_b,
                pair_gates(unswap(dg_a), idx_a), pair_gates(unswap(dg_b), idx_b))

    in_specs = (token_spec,) * 6 + layer_specs + layer_specs
    out_specs = (token_spec, token_spec) + (grad_spec,) * 6 + (token_spec, token_spec)
    return jax.shard_map(device_step, mesh=mesh, in_specs=in_specs, out_specs=out_specs, check_vma=False)
```

```python
import functools
import math
from types import SimpleNamespace

import jax
import jax.numpy as jnp
from jax import lax
from jax.experimental import pallas as pl
from jax.experimental.pallas import tpu as pltpu
from jax.sharding import PartitionSpec as P

MESH = pl.DeviceIdType.MESH
F32, BF16 = jnp.float32, jnp.bfloat16
NT = (((1,), (1,)), ((), ()))
VMEM_LIMIT = 62914560
PAIR = (0, 1)
SIDES = (1, -1)


def dev(i):
    return {'ep': i}


class Torus:
    def __init__(self, n):
        self.nx = math.isqrt(n // 2)
        self.ny = n // 2 // self.nx
        self.me = lax.axis_index('ep')
        self.c = lax.rem(self.me, 2)
        chip = self.me // 2
        self.x, self.y = lax.rem(chip, self.nx), chip // self.nx

    def at(self, dx, dy, c=None):
        x = lax.rem(self.x + dx + self.nx, self.nx)
        y = lax.rem(self.y + dy + self.ny, self.ny)
        return (y * self.nx + x) * 2 + (self.c if c is None else c)


def barrier_all(n):
    me = lax.axis_index('ep')
    b = pltpu.get_barrier_semaphore()

    def body(k, _):
        pl.semaphore_signal(b, inc=1, device_id=dev(lax.rem(me + k, n)), device_id_type=MESH)
        return 0

    lax.fori_loop(1, n, body, 0)
    pl.semaphore_wait(b, n - 1)


def remote(src, dst, ssem, rsem, to):
    return pltpu.make_async_remote_copy(src_ref=src, dst_ref=dst, send_sem=ssem, recv_sem=rsem,
                                        device_id=dev(to), device_id_type=MESH)


def barrier_some(partners):
    b = pltpu.get_barrier_semaphore()
    for p in partners:
        pl.semaphore_signal(b, inc=1, device_id=dev(p), device_id_type=MESH)
    pl.semaphore_wait(b, len(partners))


def around(t, cores):
    steps = [hops(h, d) for h in PAIR for d in SIDES]
    return [t.at(*o, c) for o in steps for c in cores] + [t.at(0, 0, 1 - t.c)]


def run_kernel(body, cid, ins, outs, scratch):
    names = [*ins, *outs, *scratch]

    def kernel(*refs):
        body(SimpleNamespace(**dict(zip(names, refs))))

    spec = lambda space: pl.BlockSpec(memory_space=space)
    res = pl.pallas_call(
        kernel,
        out_shape=[jax.ShapeDtypeStruct(shape, dtype) for shape, dtype, _ in outs.values()],
        in_specs=[spec(space) for _, space in ins.values()],
        out_specs=[spec(space) for _, _, space in outs.values()],
        scratch_shapes=list(scratch.values()),
        compiler_params=pltpu.CompilerParams(collective_id=cid, has_side_effects=True, vmem_limit_bytes=VMEM_LIMIT),
    )(*[array for array, _ in ins.values()])
    return SimpleNamespace(**dict(zip(outs, res)))


RING = 4
HBM, VMEM = pl.ANY, pltpu.VMEM
dma = pltpu.SemaphoreType.DMA


def hops(h, d, e=0):
    return (d, e) if h == 0 else (e, d)


class Gather:
    def __init__(self, torus, r, rows):
        self.t, self.block, self.out, self.ssem, self.rsem, self.lsem = torus, r.block, r.gathered, r.gs, r.gr, r.gl
        self.half, self.quarter = rows // 2, rows // 4
        self.count, self.sent, self.sibling, self.m = 0, [], [], {}

    def ref(self, off, r0, nr, core=None):
        return self.out.at[self.t.at(*off, core), pl.ds(r0, nr), :]

    def send(self, off, r0, nr, to):
        i = self.count
        self.count += 1
        ref = self.ref(off, r0, nr)
        src = self.block.at[pl.ds(r0, nr), :] if off == (0, 0) else ref
        cp = remote(src, ref, self.ssem.at[i], self.rsem.at[i], to)
        cp.start()
        self.sent.append(cp)
        return i

    def move(self, off, r0, nr, to):
        return self.send(off, r0, nr, self.t.at(*to)), nr

    def arrive(self, ref, i):
        remote(ref, ref, self.ssem.at[i], self.rsem.at[i], self.t.at(1, 0)).wait_recv()

    def wait(self, off, r0, mv):
        self.arrive(self.ref(off, r0, mv[1]), mv[0])

    def to_sibling(self, off, r0, nr):
        self.sibling.append((off, r0, nr, self.send(off, r0, nr, self.t.at(0, 0, 1 - self.t.c))))

    def start(self):
        m, half = self.m, self.half
        for h in PAIR:
            for d in SIDES:
                m[h, 'own', d] = self.move((0, 0), h * half, half, hops(h, d))
        for h in PAIR:
            for d in SIDES:
                m[h, 0, d] = self.move((0, 0), h * half, half, hops(h, 0, d))
        self.to_sibling((0, 0), 0, half * 2)
        self.own = pltpu.make_async_copy(self.block, self.out.at[self.t.me], self.lsem.at[0])
        self.own.start()

    def across(self, h, b):
        for k, e in enumerate(SIDES):
            off = hops(h, b, -e)
            self.wait(off, h * self.half, self.m[h, b, e])
            self.m[h, b, e, 'on'] = self.move(off, h * self.half + k * self.quarter, self.quarter, hops(h, 0, e))
            self.to_sibling(off, h * self.half, self.half)

    def spread(self, h, b):
        for e in SIDES:
            self.m[h, b, e] = self.move(hops(h, b), h * self.half, self.half, hops(h, 0, e))
        self.to_sibling(hops(h, b), h * self.half, self.half)

    def run(self, work=None):
        m, half, q = self.m, self.half, self.quarter
        for h in PAIR:
            for k, d in enumerate(SIDES):
                self.wait(hops(h, -d), h * half, m[h, 'own', d])
                m[h, 'on', d] = self.move(hops(h, -d), h * half + k * q, q, hops(h, d))
                self.spread(h, -d)
        for h in PAIR:
            self.across(h, 0)
        for h in PAIR:
            for k, d in enumerate(SIDES):
                self.wait(hops(h, -2 * d), h * half + k * q, m[h, 'on', d])
            self.spread(h, 2)
        if work:
            work()
        for b in (-1, 1, 2):
            for h in PAIR:
                self.across(h, b)
        for b in (0, -1, 1, 2):
            for h in PAIR:
                for k, e in enumerate(SIDES):
                    self.wait(hops(h, b, -2 * e), h * half + k * q, m[h, b, e, 'on'])
                self.to_sibling(hops(h, b, 2), h * half, half)

    def finish(self):
        for off, r0, nr, i in self.sibling:
            self.arrive(self.ref(off, r0, nr, 1 - self.t.c), i)
        for cp in self.sent:
            cp.wait_send()
        self.own.wait()


def gather_parts(block, n):
    sems = dma((80,))
    return ({'block': (block, HBM)}, {'gathered': ((n,) + block.shape, block.dtype, HBM)},
            {'gs': sems, 'gr': sems, 'gl': dma((1,))})


class Exchange:
    def __init__(self, t, n, src, dst, sems):
        self.t, self.n, self.src, self.dst = t, n, src, dst
        self.ss, self.rs, self.ls = sems

    def send(self, k):
        to = lax.rem(self.t.me + k, self.n)
        return remote(self.src(to), self.dst.at[self.t.me], self.ss.at[k], self.rs.at[k], to)

    def start(self):
        def body(k, _):
            self.send(k).start()
            return 0

        self.own = pltpu.make_async_copy(self.src(self.t.me), self.dst.at[self.t.me], self.ls.at[0])
        self.own.start()
        lax.fori_loop(1, self.n, body, 0)

    def finish(self):
        def body(k, _):
            fr = lax.rem(self.t.me - k + self.n, self.n)
            remote(self.src(fr), self.dst.at[fr], self.ss.at[k], self.rs.at[k], fr).wait_recv()
            self.send(k).wait_send()
            return 0

        lax.fori_loop(1, self.n, body, 0)
        self.own.wait()


class Tables:
    def __init__(self, t, n, r):
        self.t, self.r = t, r
        flat = lambda i: r.g.at[i // (2 * t.nx), lax.rem(i // 2, t.nx), lax.rem(i, 2)]
        self.experts = Exchange(t, n, flat, r.g_recv, (r.ts, r.tr, r.tl))

    def start(self):
        t, r = self.t, self.r
        self.own = [pltpu.make_async_copy(r.g.at[t.y], r.by_x.at[t.y], r.tl.at[1]),
                    pltpu.make_async_copy(r.g.at[:, t.x], r.by_y.at[t.x], r.tl.at[2])]
        for cp in self.own:
            cp.start()
        self.lines = []
        for d in range(1, RING):
            y, x = lax.rem(t.y + d, RING), lax.rem(t.x + d, RING)
            fy, fx = lax.rem(t.y + RING - d, RING), lax.rem(t.x + RING - d, RING)
            for h, src, dst, me, fr in ((1, r.g.at[y], r.by_x, t.y, fy), (0, r.g.at[:, x], r.by_y, t.x, fx)):
                self.lines += [remote(src, dst.at[i], r.us.at[h, d], r.ur.at[h, d], t.at(*hops(h, d))) for i in (me, fr)]
        for cp in self.lines[::2]:
            cp.start()
        self.experts.start()

    def finish(self):
        self.experts.finish()
        for cp, arrival in zip(self.lines[::2], self.lines[1::2]):
            arrival.wait_recv()
            cp.wait_send()
        for cp in self.own:
            cp.wait()


CHUNK = 512


class Shared:
    def __init__(self, r):
        self.r = r
        self.copies = [pltpu.make_async_copy(a, b, r.wl.at[i])
                       for i, (a, b) in enumerate(((r.ws1, r.v1), (r.ws3, r.v3), (r.ws2, r.v2)))]
        for cp in self.copies:
            cp.start()

    def ready(self):
        for cp in self.copies:
            cp.wait()

    def loop(self, out, step):
        out[...] = jnp.zeros_like(out)

        def body(i, _):
            out[...] += step(pl.ds(pl.multiple_of(i * CHUNK, CHUNK), CHUNK))
            return 0

        lax.fori_loop(0, self.r.v1.shape[1] // CHUNK, body, 0)

    def forward(self, x_t, out):
        r, x = self.r, x_t.T

        def step(at):
            return mm_nt(r.v2[:, at], hidden_of(mm(x, r.v1[:, at]), mm(x, r.v3[:, at]))[1])

        self.loop(out, step)

    def backward(self, x_t, dy_t, out):
        r, x, dy = self.r, x_t.T, dy_t.T

        def step(at):
            a1, a3 = mm(x, r.v1[:, at]), mm(x, r.v3[:, at])
            da1, da3 = swiglu_grads(a1, a3, mm(dy, r.v2[:, at]))
            return mm_nt(r.v1[:, at], da1) + mm_nt(r.v3[:, at], da3)

        self.loop(out, step)


def shared_parts(ws1, ws3, ws2):
    buf = VMEM(ws1.shape, BF16)
    return ({'ws1': (ws1, HBM), 'ws3': (ws3, HBM), 'ws2': (ws2.T, HBM)},
            {'v1': buf, 'v3': buf, 'v2': buf, 'wl': dma((3,))})


def gather_first(x_t, g, weights, n, cid):
    tokens = g.shape[2]
    side = math.isqrt(n // 2)
    line = ((side, side, 2, 8, tokens), F32, HBM)
    ins, outs, scratch = gather_parts(x_t, n)
    w_ins, w_scratch = shared_parts(*weights)
    table, lines = dma((n,)), dma((2, RING))

    def body(r):
        t = Torus(n)
        shared = Shared(r)
        barrier_all(n)
        gather, tables = Gather(t, r, x_t.shape[0]), Tables(t, n, r)
        gather.start()
        tables.start()
        shared.ready()
        shared.forward(r.x[...], r.s)
        gather.run()
        tables.finish()
        gather.finish()

    res = run_kernel(body, cid, {**ins, **w_ins, 'g': (g.reshape(line[0]), HBM), 'x': (x_t, VMEM)},
                     {**outs, 'g_recv': ((n, 8, tokens), F32, HBM), 'by_x': line, 'by_y': line,
                      's': (x_t.shape, F32, VMEM)},
                     {**scratch, **w_scratch, 'ts': table, 'tr': table, 'tl': dma((3,)), 'us': lines, 'ur': lines})
    return res.gathered, res.g_recv, [a.reshape(side, 2 * side, 8, tokens) for a in (res.by_x, res.by_y)], res.s


def gather_second(block, weights, n, cid):
    ins, outs, scratch = gather_parts(block, n)
    w_ins, w_scratch = shared_parts(*weights)
    d = block.shape[0] // 2
    part = ((d, block.shape[1]), F32, VMEM)

    def body(r):
        t = Torus(n)
        shared = Shared(r)
        barrier_some(around(t, [t.c]))
        gather = Gather(t, r, block.shape[0])
        gather.start()
        shared.ready()
        shared.forward(r.x[:d], r.s)
        gather.run(lambda: shared.backward(r.x[:d], r.x[d:], r.ds))
        gather.finish()

    res = run_kernel(body, cid, {**ins, **w_ins, 'x': (block, VMEM)}, {**outs, 's': part, 'ds': part},
                     {**scratch, **w_scratch})
    return res.gathered, res.s, res.ds


def gather_third(block, n, cid):
    ins, outs, scratch = gather_parts(block, n)

    def body(r):
        t = Torus(n)
        barrier_some(around(t, [t.c]))
        gather = Gather(t, r, block.shape[0])
        gather.start()
        gather.run()
        gather.finish()

    return run_kernel(body, cid, ins, outs, scratch).gathered


def mm(a, b):
    return jnp.dot(a, b, preferred_element_type=F32)


def mm_nt(a, b):
    return lax.dot_general(a, b, NT, preferred_element_type=F32)


def slots_of(gates):
    tokens = gates.shape[1]
    before = (lax.broadcasted_iota(jnp.int32, (tokens, tokens), 0)
              < lax.broadcasted_iota(jnp.int32, (tokens, tokens), 1))
    member = gates > 0.0
    count = mm(jnp.where(member, 1.0, 0.0).astype(BF16), jnp.where(before, 1.0, 0.0).astype(BF16))
    return jnp.where(member, count, -1.0)


def pick(slot_rows, capacity):
    tokens = slot_rows[0].shape[1]
    want = lax.broadcasted_iota(jnp.int32, (capacity, tokens), 0).astype(F32)
    return jnp.concatenate([jnp.where(s == want, 1.0, 0.0) for s in slot_rows], axis=0)


def split3(v):
    a = v.astype(BF16).astype(F32)
    r = v - a
    b = r.astype(BF16).astype(F32)
    return a, b, r - b


def swap_halves(first, second):
    low = lax.broadcasted_iota(jnp.int32, first.shape, 1) < first.shape[1] // 2
    return jnp.where(low, first, second), jnp.where(low, second, first)


def hidden_of(a1, a3):
    sigma = jax.nn.sigmoid(a1)
    return sigma, (a1 * sigma * a3).astype(BF16)


def source_hot(slots, s, row, capacity):
    return pick([slots[8 * s + row:8 * s + row + 1], slots[8 * s + row + 1:8 * s + row + 2]], capacity).astype(BF16)


def pair_rows(block, p, slots, row, capacity):
    return swap_halves(*[mm_nt(block[s], source_hot(slots, s, row, capacity)) for s in (2 * p, 2 * p + 1)])


def forward_kernel(row, capacity, keep, x_ref, g_ref, w1_ref, w3_ref, w2_ref, *outs):
    o_ref, w2t = outs[0], outs[-1]
    sources = x_ref.shape[0]

    @pl.when(pl.program_id(0) == 0)
    def _():
        for e in PAIR:
            w2t[e] = w2_ref[e].T

    slots = slots_of(g_ref[...].reshape(sources * 8, -1))
    pairs = [pair_rows(x_ref, p, slots, row, capacity) for p in range(sources // 2)]
    o = []
    for e in PAIR:
        rows = jnp.concatenate([pr[e].astype(BF16) for pr in pairs], axis=1)
        if keep:
            outs[1][e] = rows
        hidden = hidden_of(mm(w1_ref[e], rows), mm(w3_ref[e], rows))[1]
        o.append(mm(w2t[e], hidden))
    width = 2 * capacity
    for p in range(sources // 2):
        a, b = swap_halves(o[0][:, p * width:(p + 1) * width], o[1][:, p * width:(p + 1) * width])
        o_ref[2 * p] = a.astype(BF16)
        o_ref[2 * p + 1] = b.astype(BF16)


def backward_kernel(row, capacity, kept, x_ref, dy_ref, g_ref, w1_ref, w3_ref, w2_ref,
                    dw1_ref, dw3_ref, dw2_ref, du_ref, gg_ref, w1n, w3n):
    sources = dy_ref.shape[0]

    @pl.when(pl.program_id(0) == 0)
    def _():
        for ref in (dw1_ref, dw3_ref, dw2_ref):
            ref[...] = jnp.zeros_like(ref)
        for e in PAIR:
            w1n[e] = w1_ref[e].T
            w3n[e] = w3_ref[e].T

    d, tokens = dy_ref.shape[1:]
    width = 2 * capacity
    slots = slots_of(g_ref[...].reshape(sources * 8, -1))
    low = lax.broadcasted_iota(jnp.int32, (1, width), 1) < capacity
    if not kept:
        xp = [pair_rows(x_ref, p, slots, row, capacity) for p in range(sources // 2)]
    hots, dyp, gp = [], [], []
    for p in range(sources // 2):
        raw, gates = [], []
        for s in (2 * p, 2 * p + 1):
            hot = source_hot(slots, s, row, capacity)
            hots.append(hot)
            parts = split3(g_ref[s])
            extra = jnp.concatenate(list(parts) + [jnp.zeros_like(parts[0])], axis=0).astype(BF16)
            r = mm_nt(jnp.concatenate([dy_ref[s], extra], axis=0), hot)
            raw.append(r[:d])
            both = [r[d + i:d + i + 1] + r[d + 8 + i:d + 9 + i] + r[d + 16 + i:d + 17 + i] for i in (row, row + 1)]
            gates.append(jnp.where(low, *both))
        dyp.append(swap_halves(*raw))
        gp.append(swap_halves(*gates))
    du, gg = [], []
    for e in PAIR:
        rows = x_ref[e] if kept else jnp.concatenate([pr[e].astype(BF16) for pr in xp], axis=1)
        dy = jnp.concatenate([pr[e] for pr in dyp], axis=1)
        gate = jnp.concatenate([pr[e] for pr in gp], axis=1)
        a1, a3 = mm(w1_ref[e], rows), mm(w3_ref[e], rows)
        sigma, hidden = hidden_of(a1, a3)
        p32 = mm(w2_ref[e], dy.astype(BF16))
        gg.append(jnp.sum(hidden.astype(F32) * p32, axis=0, keepdims=True))
        dw2_ref[e] += mm_nt(hidden, (gate * dy).astype(BF16))
        q = gate * p32
        da1 = (q * a3 * sigma * (1.0 + a1 * (1.0 - sigma))).astype(BF16)
        da3 = (q * a1 * sigma).astype(BF16)
        dw1_ref[e] += mm_nt(da1, rows)
        dw3_ref[e] += mm_nt(da3, rows)
        du.append(mm(w1n[e], da1) + mm(w3n[e], da3))
    for p in range(sources // 2):
        at = slice(p * width, (p + 1) * width)
        for s, v in zip((2 * p, 2 * p + 1), swap_halves(du[0][:, at], du[1][:, at])):
            du_ref[s] = v.astype(BF16)
        for s, v in zip((2 * p, 2 * p + 1), swap_halves(gg[0][:, at], gg[1][:, at])):
            wide = jnp.broadcast_to(v, (8, width))
            own = (lax.broadcasted_iota(jnp.int32, (8, width), 1) // capacity
                   == lax.broadcasted_iota(jnp.int32, (8, width), 0))
            parts = split3(jnp.where(own, wide, 0.0))
            res = mm(jnp.concatenate(list(parts) + [jnp.zeros_like(parts[0])], axis=0).astype(BF16), hots[s])
            gg_ref[s] = (res[:8] + res[8:16] + res[16:24])[:gg_ref.shape[1]]


SOURCES = 4


def whole(a):
    return pl.BlockSpec(a.shape, lambda i: (0,) * a.ndim)


def experts_forward(xg, gr, w1, w3, w2, row, capacity, keep):
    n, d, tokens = xg.shape[0], w1.shape[2], xg.shape[2]
    lanes = SOURCES * capacity
    out_shape = [jax.ShapeDtypeStruct((n, d, 2 * capacity), BF16)]
    out_specs = [pl.BlockSpec((SOURCES, d, 2 * capacity), lambda i: (i, 0, 0))]
    if keep:
        out_shape.append(jax.ShapeDtypeStruct((2, d, n * capacity), BF16))
        out_specs.append(pl.BlockSpec((2, d, lanes), lambda i: (0, 0, i)))
    return pl.pallas_call(
        functools.partial(forward_kernel, row, capacity, keep),
        grid=(n // SOURCES,),
        out_shape=out_shape, out_specs=out_specs,
        in_specs=[pl.BlockSpec((SOURCES, d, tokens), lambda i: (i, 0, 0)),
                  pl.BlockSpec((SOURCES, 8, tokens), lambda i: (i, 0, 0)), whole(w1), whole(w3), whole(w2)],
        scratch_shapes=[pltpu.VMEM((2, d, w2.shape[1]), BF16)],
        compiler_params=pltpu.CompilerParams(vmem_limit_bytes=VMEM_LIMIT),
    )(xg, gr, w1, w3, w2)


def experts_backward(x, dyg, gr, w1, w3, w2, row, capacity, kept):
    n, d, tokens = dyg.shape[0], w1.shape[2], dyg.shape[2]
    lanes = SOURCES * capacity
    f = w2.shape[1]
    grouped = lambda i: (i, 0, 0)
    x_spec = (pl.BlockSpec((2, d, lanes), lambda i: (0, 0, i)) if kept
              else pl.BlockSpec((SOURCES, d, tokens), grouped))
    grads = [jax.ShapeDtypeStruct((2, f, d), F32)] * 3
    return pl.pallas_call(
        functools.partial(backward_kernel, row, capacity, kept),
        grid=(n // SOURCES,),
        out_shape=grads + [jax.ShapeDtypeStruct((n, d, 2 * capacity), BF16),
                           jax.ShapeDtypeStruct((n, 2, tokens), F32)],
        out_specs=[whole(g) for g in grads] + [pl.BlockSpec((SOURCES, d, 2 * capacity), grouped),
                                               pl.BlockSpec((SOURCES, 2, tokens), grouped)],
        in_specs=[x_spec, pl.BlockSpec((SOURCES, d, tokens), lambda i: (i, 1, 0)),
                  pl.BlockSpec((SOURCES, 8, tokens), grouped), whole(w1), whole(w3), whole(w2)],
        scratch_shapes=[pltpu.VMEM((2, d, f), BF16), pltpu.VMEM((2, d, f), BF16)],
        compiler_params=pltpu.CompilerParams(vmem_limit_bytes=VMEM_LIMIT),
    )(x, dyg, gr, w1, w3, w2)


FAR_TO_NEAR = (2, 1, -1, 0)
ROUND_SEMS = 8


class Return:
    def __init__(self, torus, r, name, row, capacity, gated):
        self.t, self.row, self.capacity, self.gated = torus, row, capacity, gated
        for field in ('src', 'out', *RETURN_SCRATCH):
            setattr(self, field, getattr(r, name + field))
        self.tables = (r.by_x, r.by_y)
        self.half = self.src.shape[3] // 2
        self.quarter = self.half // 2
        self.sent = []

    def pos(self, h):
        return (self.t.x, self.t.y) if h == 0 else (self.t.y, self.t.x)

    def source(self, h, p, q, cores):
        rows = pl.ds(h * self.half, self.half)
        a, b = (q, p) if h == 0 else (p, q)
        return self.src.at[a, b, cores, rows, :]

    def push(self, src, dst, h, j, slot, to, second=False):
        ss, rs = (self.ss2, self.rs2) if second else (self.ss, self.rs)
        at = (h, slot) if second else (h, j, slot)
        cp = remote(src, dst, ss.at[at], rs.at[at], to)
        cp.start()
        self.sent.append(cp)

    def arrive(self, dst, h, j, slot, second=False):
        ss, rs = (self.ss2, self.rs2) if second else (self.ss, self.rs)
        at = (h, slot) if second else (h, j, slot)
        remote(dst, dst, ss.at[at], rs.at[at], self.t.at(1, 0)).wait_recv()

    def turn(self, j):
        return 1 if j % 2 == 0 else -1

    def sends(self, j):
        c = self.t.c
        for h in PAIR:
            p, q0 = self.pos(h)
            q = lax.rem(q0 + FAR_TO_NEAR[j] + RING, RING)
            d = self.turn(j)
            self.push(self.source(h, lax.rem(p + 2, RING), q, slice(None)), self.relay.at[h, j], h, j, 0,
                      self.t.at(*hops(h, d)))
            k = p * 2 + c
            for i, d in enumerate(SIDES):
                for core in PAIR:
                    self.direct(h, j, i, d, core, p, q, k)
            self.push(self.source(h, p, q, 1 - c), self.recv.at[h, j, k], h, j, 5, self.t.at(0, 0, 1 - c))
            pltpu.make_async_copy(self.source(h, p, q, c), self.recv.at[h, j, k], self.ls.at[h, j]).start()

    def direct(self, h, j, i, d, core, p, q, k):
        cp = remote(self.source(h, lax.rem(p + d + RING, RING), q, core), self.recv.at[h, j, k],
                    self.ss.at[h, j, 1 + i * 2 + core], self.rs.at[h, j, 1 + i * 2 + self.t.c],
                    self.t.at(*hops(h, d), core))
        cp.start()
        self.sent.append(cp)

    def forward(self, j):
        c, d = self.t.c, self.turn(j)
        for h in PAIR:
            p, _ = self.pos(h)
            self.arrive(self.relay.at[h, j], h, j, 0)
            k = lax.rem(p - d + RING, RING) * 2 + c
            for core in PAIR:
                cp = remote(self.relay.at[h, j, core], self.recv.at[h, j, k], self.ss.at[h, j, 6 + core],
                            self.rs.at[h, j, 6 + c], self.t.at(*hops(h, d), core))
                cp.start()
                self.sent.append(cp)

    def arrivals(self, j):
        for h in PAIR:
            p, q0 = self.pos(h)
            for slot in (1, 2, 3, 4, 5, 6, 7):
                self.arrive(self.recv.at[h, j, 0], h, j, slot)
            q = lax.rem(q0 + FAR_TO_NEAR[j] + RING, RING)
            pltpu.make_async_copy(self.source(h, p, q, self.t.c), self.recv.at[h, j, 0], self.ls.at[h, j]).wait()

    def combine(self, h, j):
        _, q0 = self.pos(h)
        q = lax.rem(q0 + FAR_TO_NEAR[j] + RING, RING)
        gates = self.tables[h][q]
        senders, _, tokens = gates.shape
        slots = slots_of(gates.reshape(senders * 8, tokens))
        acc = None
        for m in range(senders // 2):
            ks = (2 * m, 2 * m + 1)
            lhs = jnp.concatenate([self.recv[h, j, k] for k in ks], axis=1)
            order = [8 * k + self.row + e for k in ks for e in PAIR]
            hot = pick([slots[r:r + 1] for r in order], self.capacity)
            if self.gated:
                parts = [split3(gates[k, self.row + e:self.row + e + 1]) for k in ks for e in PAIR]
                weights = [hot * jnp.concatenate([jnp.broadcast_to(g[i], (self.capacity, tokens)) for g in parts], axis=0)
                           for i in range(3)]
            else:
                weights = [hot]
            for w in weights:
                term = mm(lhs, w.astype(BF16))
                acc = term if acc is None else acc + term
        return acc

    def round(self, j):
        half, quarter = self.half, self.quarter
        for h in PAIR:
            acc = self.combine(h, j)
            up, down = self.t.at(*hops(h, 0, 1)), self.t.at(*hops(h, 0, -1))
            mine = self.part.at[h, j]
            if j == 0:
                self.part[h, j] = acc
                self.push(mine.at[pl.ds(0, quarter)], self.rin.at[h, 0], h, j, 0, up, True)
                self.push(mine.at[pl.ds(quarter, quarter)], self.rin.at[h, 1], h, j, 1, down, True)
            elif j == 1:
                self.arrive(self.rin.at[h, 0], h, j, 0, True)
                self.part[h, j, :quarter] = acc[:quarter] + self.rin[h, 0]
                self.part[h, j, quarter:] = acc[quarter:]
                self.push(mine, self.fin.at[h, 0], h, j, 2, up, True)
            elif j == 2:
                self.arrive(self.rin.at[h, 1], h, j, 1, True)
                self.part[h, j, :quarter] = acc[:quarter]
                self.part[h, j, quarter:] = acc[quarter:] + self.rin[h, 1]
                self.push(mine, self.fin.at[h, 1], h, j, 3, down, True)
            else:
                self.out[h * half:(h + 1) * half, :] = acc

    def finish(self):
        for h in PAIR:
            for i in PAIR:
                self.arrive(self.fin.at[h, i], h, 0, 2 + i, True)
            at = slice(h * self.half, (h + 1) * self.half)
            self.out[at, :] = self.out[at, :] + self.fin[h, 0] + self.fin[h, 1]
        for cp in self.sent:
            cp.wait_send()


RETURN_SCRATCH = ('recv', 'relay', 'part', 'rin', 'fin', 'ss', 'rs', 'ss2', 'rs2', 'ls')


def return_parts(name, rows, tokens, n):
    d, width = rows.shape[1:]
    side = math.isqrt(n // 2)
    half = d // 2
    first, second = dma((2, RING, ROUND_SEMS)), dma((2, RING))
    shapes = (VMEM((2, RING, 2 * RING, half, width), BF16), VMEM((2, RING, 2, half, width), BF16),
              VMEM((2, RING, half, tokens), F32), VMEM((2, 2, half // 2, tokens), F32),
              VMEM((2, 2, half, tokens), F32), first, first, second, second, second)
    return ({name + 'src': (rows.reshape(side, side, 2, d, width), HBM)},
            {**{name + f: shape for f, shape in zip(RETURN_SCRATCH, shapes)}, name + 'out': VMEM((d, tokens), F32)})


def drive(todo, work=None):
    steps = [(r, j) for r in todo for j in range(RING)]
    for r, j in steps[:2]:
        r.sends(j)
    todo[0].forward(0)
    if work:
        work()
    for u, (r, j) in enumerate(steps):
        for later, k in steps[u + 2:u + 3]:
            later.sends(k)
        for later, k in steps[u + 1:u + 2]:
            later.forward(k)
        r.arrivals(j)
        r.round(j)
    for r in todo:
        r.finish()


def gg_parts(gg, n):
    sems = dma((n,))
    return {'gg': (gg, HBM)}, {'dg': (gg.shape, F32, HBM)}, {'qs': sems, 'qr': sems, 'ql': dma((1,))}


def return_first(o, lines, x_t, s, dy_t, row, capacity, n, cid):
    d, tokens = x_t.shape
    ins, scratch = return_parts('o', o, tokens, n)

    def body(r):
        t = Torus(n)
        barrier_some(around(t, PAIR))
        job = Return(t, r, 'o', row, capacity, True)
        drive([job])
        r.block[:d] = (r.x[...].astype(F32) + r.s[...] + job.out[...]).astype(BF16)
        r.block[d:] = r.dy[...]

    return run_kernel(body, cid, {**ins, 'by_x': (lines[0], VMEM), 'by_y': (lines[1], VMEM), 'x': (x_t, VMEM),
                                  's': (s, VMEM), 'dy': (dy_t, VMEM)},
                      {'block': ((2 * d, tokens), BF16, VMEM)}, scratch).block


def return_second(du, o, gg, lines, block, s, ds, x_t, row, capacity, n, cid):
    d, tokens = x_t.shape
    u_ins, u_scratch = return_parts('u', du, tokens, n)
    o_ins, o_scratch = return_parts('o', o, tokens, n)
    g_ins, g_outs, g_scratch = gg_parts(gg, n)

    def body(r):
        t = Torus(n)
        barrier_all(n)
        back = Exchange(t, n, lambda i: r.gg.at[i], r.dg, (r.qs, r.qr, r.ql))
        back.start()
        u, o = Return(t, r, 'u', row, capacity, False), Return(t, r, 'o', row, capacity, True)
        drive([u, o])
        r.last[...] = (r.x1dy[:d].astype(F32) + r.s[...] + o.out[...]).astype(BF16)
        r.block[:d] = r.x[...]
        r.block[d:] = (r.x1dy[d:].astype(F32) + r.ds[...] + u.out[...]).astype(BF16)
        back.finish()

    res = run_kernel(body, cid, {**u_ins, **o_ins, **g_ins, 'by_x': (lines[0], VMEM), 'by_y': (lines[1], VMEM),
                                 'x1dy': (block, VMEM), 's': (s, VMEM), 'ds': (ds, VMEM), 'x': (x_t, VMEM)},
                     {**g_outs, 'last': (x_t.shape, BF16, VMEM), 'block': (block.shape, BF16, VMEM)},
                     {**u_scratch, **o_scratch, **g_scratch})
    return res.last, res.block, res.dg


def return_third(du, gg, lines, block, weights, row, capacity, n, cid):
    d, tokens = block.shape[0] // 2, block.shape[1]
    ins, scratch = return_parts('u', du, tokens, n)
    g_ins, g_outs, g_scratch = gg_parts(gg, n)
    w_ins, w_scratch = shared_parts(*weights)

    def body(r):
        t = Torus(n)
        shared = Shared(r)
        barrier_all(n)
        back = Exchange(t, n, lambda i: r.gg.at[i], r.dg, (r.qs, r.qr, r.ql))
        back.start()
        u = Return(t, r, 'u', row, capacity, False)

        def work():
            shared.ready()
            shared.backward(r.xdy[:d], r.xdy[d:], r.ds)

        drive([u], work)
        r.dx[...] = (r.xdy[d:].astype(F32) + r.ds[...] + u.out[...]).astype(BF16)
        back.finish()

    res = run_kernel(body, cid, {**ins, **g_ins, **w_ins, 'by_x': (lines[0], VMEM), 'by_y': (lines[1], VMEM),
                                 'xdy': (block, VMEM)},
                     {**g_outs, 'dx': ((d, tokens), BF16, VMEM)},
                     {**scratch, **g_scratch, **w_scratch, 'ds': VMEM((d, tokens), F32)})
    return res.dx, res.dg


def swiglu_grads(pre_gate, pre_up, d_hidden):
    sigma = jax.nn.sigmoid(pre_gate)
    d_gate = d_hidden * pre_up * sigma * (1.0 + pre_gate * (1.0 - sigma))
    d_up = d_hidden * pre_gate * sigma
    return d_gate.astype(BF16), d_up.astype(BF16)


def gate_table(idx, gate, n_experts):
    ids = jnp.arange(n_experts, dtype=idx.dtype)[:, None, None]
    return jnp.sum(jnp.where(idx.T[None] == ids, gate.T[None], 0.0), axis=1)


def pair_gates(dg, idx):
    ids = jnp.arange(dg.shape[0], dtype=idx.dtype)[:, None, None]
    return jnp.sum(jnp.where(idx.T[None] == ids, dg[:, None, :], 0.0), axis=0).T


def solution(mesh):
    n = mesh.shape['ep']
    token_spec = P(('dp', 'ep'), None)
    expert_spec = P('ep', None, None)
    shared_spec = P(None, None)
    grad_spec = P(('dp', 'ep'), None, None)
    layer_specs = (expert_spec,) * 3 + (shared_spec,) * 3

    def device_step(x_in, d_out, idx_a, gate_a, idx_b, gate_b,
                    w1_a, w3_a, w2_a, ws1_a, ws3_a, ws2_a,
                    w1_b, w3_b, w2_b, ws1_b, ws3_b, ws2_b):
        tokens, top_k = idx_a.shape
        n_experts = w1_a.shape[0] * n
        capacity = top_k * ((2 * tokens + n_experts - 1) // n_experts)

        flip = lambda w: jnp.swapaxes(w, 1, 2)
        w1_a, w3_a, w1_b, w3_b = flip(w1_a), flip(w3_a), flip(w1_b), flip(w3_b)

        odd = lax.rem(lax.axis_index('ep'), 2) == 1
        tables = [gate_table(i, g, n_experts).reshape(n, 2, tokens) for i, g in ((idx_a, gate_a), (idx_b, gate_b))]
        tables = [jnp.where(odd, t[:, ::-1], t) for t in tables]
        g_own = jnp.concatenate(tables + [jnp.zeros((n, 4, tokens), F32)], axis=1)

        x_t, dy_t = x_in.T, d_out.T
        shared_a, shared_b = (ws1_a, ws3_a, ws2_a), (ws1_b, ws3_b, ws2_b)
        xg, g_recv, lines, s_a = gather_first(x_t, g_own, shared_a, n, 0)
        (o_a,) = experts_forward(xg, g_recv, w1_a, w3_a, w2_a, 0, capacity, False)
        block = return_first(o_a, lines, x_t, s_a, dy_t, 0, capacity, n, 1)

        both, s_b, ds_b = gather_second(block, shared_b, n, 2)
        o_b, rows_b = experts_forward(both, g_recv, w1_b, w3_b, w2_b, 2, capacity, True)
        dw1_b, dw3_b, dw2_b, du_b, gg_b = experts_backward(rows_b, both, g_recv, w1_b, w3_b, w2_b, 2, capacity, True)
        x_last, block, dg_b = return_second(du_b, o_b, gg_b, lines, block, s_b, ds_b, x_t, 2, capacity, n, 3)

        both = gather_third(block, n, 4)
        dw1_a, dw3_a, dw2_a, du_a, gg_a = experts_backward(both, both, g_recv, w1_a, w3_a, w2_a, 0, capacity, False)
        d_first, dg_a = return_third(du_a, gg_a, lines, block, shared_a, 0, capacity, n, 5)
        x_last, d_first = x_last.T, d_first.T

        def unswap(dg):
            return jnp.where(odd, dg[:, ::-1], dg).reshape(2 * n, tokens)

        return (x_last, d_first, flip(dw1_a), flip(dw3_a), dw2_a, flip(dw1_b), flip(dw3_b), dw2_b,
                pair_gates(unswap(dg_a), idx_a), pair_gates(unswap(dg_b), idx_b))

    in_specs = (token_spec,) * 6 + layer_specs + layer_specs
    out_specs = (token_spec, token_spec) + (grad_spec,) * 6 + (token_spec, token_spec)
    return jax.shard_map(device_step, mesh=mesh, in_specs=in_specs, out_specs=out_specs, check_vma=False)
```

```python
import functools
import math
from types import SimpleNamespace

import jax
import jax.numpy as jnp
from jax import lax
from jax.experimental import pallas as pl
from jax.experimental.pallas import tpu as pltpu
from jax.sharding import PartitionSpec as P

MESH = pl.DeviceIdType.MESH
F32, BF16 = jnp.float32, jnp.bfloat16
NT = (((1,), (1,)), ((), ()))
VMEM_LIMIT = 62914560
PAIR = (0, 1)
SIDES = (1, -1)


def dev(i):
    return {'ep': i}


class Torus:
    def __init__(self, n):
        self.nx = math.isqrt(n // 2)
        self.ny = n // 2 // self.nx
        self.me = lax.axis_index('ep')
        self.c = lax.rem(self.me, 2)
        chip = self.me // 2
        self.x, self.y = lax.rem(chip, self.nx), chip // self.nx

    def at(self, dx, dy, c=None):
        x = lax.rem(self.x + dx + self.nx, self.nx)
        y = lax.rem(self.y + dy + self.ny, self.ny)
        return (y * self.nx + x) * 2 + (self.c if c is None else c)


def barrier_all(n):
    me = lax.axis_index('ep')
    b = pltpu.get_barrier_semaphore()

    def body(k, _):
        pl.semaphore_signal(b, inc=1, device_id=dev(lax.rem(me + k, n)), device_id_type=MESH)
        return 0

    lax.fori_loop(1, n, body, 0)
    pl.semaphore_wait(b, n - 1)


def remote(src, dst, ssem, rsem, to):
    return pltpu.make_async_remote_copy(src_ref=src, dst_ref=dst, send_sem=ssem, recv_sem=rsem,
                                        device_id=dev(to), device_id_type=MESH)


def barrier_some(partners):
    b = pltpu.get_barrier_semaphore()
    for p in partners:
        pl.semaphore_signal(b, inc=1, device_id=dev(p), device_id_type=MESH)
    pl.semaphore_wait(b, len(partners))


def around(t):
    return [t.at(*hops(h, d)) for h in PAIR for d in SIDES] + [t.at(0, 0, 1 - t.c)]


def lines_of(t):
    return [t.at(*hops(h, d), c) for h in PAIR for d in (1, -1, 2) for c in PAIR] + [t.at(0, 0, 1 - t.c)]


def run_kernel(body, cid, ins, outs, scratch):
    names = [*ins, *outs, *scratch]

    def kernel(*refs):
        body(SimpleNamespace(**dict(zip(names, refs))))

    spec = lambda space: pl.BlockSpec(memory_space=space)
    res = pl.pallas_call(
        kernel,
        out_shape=[jax.ShapeDtypeStruct(shape, dtype) for shape, dtype, _ in outs.values()],
        in_specs=[spec(space) for _, space in ins.values()],
        out_specs=[spec(space) for _, _, space in outs.values()],
        scratch_shapes=list(scratch.values()),
        compiler_params=pltpu.CompilerParams(collective_id=cid, has_side_effects=True, vmem_limit_bytes=VMEM_LIMIT),
    )(*[array for array, _ in ins.values()])
    return SimpleNamespace(**dict(zip(outs, res)))


RING = 4
HBM, VMEM = pl.ANY, pltpu.VMEM
dma = pltpu.SemaphoreType.DMA


def hops(h, d, e=0):
    return (d, e) if h == 0 else (e, d)


class Gather:
    def __init__(self, torus, r, rows):
        self.t, self.block, self.out, self.ssem, self.rsem, self.lsem = torus, r.block, r.gathered, r.gs, r.gr, r.gl
        self.half, self.quarter = rows // 2, rows // 4
        self.count, self.sent, self.sibling, self.m = 0, [], [], {}

    def ref(self, off, r0, nr, core=None):
        return self.out.at[self.t.at(*off, core), pl.ds(r0, nr), :]

    def send(self, off, r0, nr, to):
        i = self.count
        self.count += 1
        ref = self.ref(off, r0, nr)
        src = self.block.at[pl.ds(r0, nr), :] if off == (0, 0) else ref
        cp = remote(src, ref, self.ssem.at[i], self.rsem.at[i], to)
        cp.start()
        self.sent.append(cp)
        return i

    def move(self, off, r0, nr, to):
        return self.send(off, r0, nr, self.t.at(*to)), nr

    def arrive(self, ref, i):
        remote(ref, ref, self.ssem.at[i], self.rsem.at[i], self.t.at(1, 0)).wait_recv()

    def wait(self, off, r0, mv):
        self.arrive(self.ref(off, r0, mv[1]), mv[0])

    def to_sibling(self, off, r0, nr):
        self.sibling.append((off, r0, nr, self.send(off, r0, nr, self.t.at(0, 0, 1 - self.t.c))))

    def start(self):
        m, half = self.m, self.half
        for h in PAIR:
            for d in SIDES:
                m[h, 'own', d] = self.move((0, 0), h * half, half, hops(h, d))
        for h in PAIR:
            for d in SIDES:
                m[h, 0, d] = self.move((0, 0), h * half, half, hops(h, 0, d))
        self.to_sibling((0, 0), 0, half * 2)
        self.own = pltpu.make_async_copy(self.block, self.out.at[self.t.me], self.lsem.at[0])
        self.own.start()

    def across(self, h, b):
        for k, e in enumerate(SIDES):
            off = hops(h, b, -e)
            self.wait(off, h * self.half, self.m[h, b, e])
            self.m[h, b, e, 'on'] = self.move(off, h * self.half + k * self.quarter, self.quarter, hops(h, 0, e))
            self.to_sibling(off, h * self.half, self.half)

    def spread(self, h, b):
        for e in SIDES:
            self.m[h, b, e] = self.move(hops(h, b), h * self.half, self.half, hops(h, 0, e))
        self.to_sibling(hops(h, b), h * self.half, self.half)

    def run(self):
        m, half, q = self.m, self.half, self.quarter
        for h in PAIR:
            for k, d in enumerate(SIDES):
                self.wait(hops(h, -d), h * half, m[h, 'own', d])
                m[h, 'on', d] = self.move(hops(h, -d), h * half + k * q, q, hops(h, d))
                self.spread(h, -d)
        for h in PAIR:
            self.across(h, 0)
        for h in PAIR:
            for k, d in enumerate(SIDES):
                self.wait(hops(h, -2 * d), h * half + k * q, m[h, 'on', d])
            self.spread(h, 2)
        for b in (-1, 1, 2):
            for h in PAIR:
                self.across(h, b)
        for b in (0, -1, 1, 2):
            for h in PAIR:
                for k, e in enumerate(SIDES):
                    self.wait(hops(h, b, -2 * e), h * half + k * q, m[h, b, e, 'on'])
                self.to_sibling(hops(h, b, 2), h * half, half)

    def finish(self):
        for off, r0, nr, i in self.sibling:
            self.arrive(self.ref(off, r0, nr, 1 - self.t.c), i)
        for cp in self.sent:
            cp.wait_send()
        self.own.wait()


def gather_parts(block, n):
    sems = dma((80,))
    return ({'block': (block, HBM)}, {'gathered': ((n,) + block.shape, block.dtype, HBM)},
            {'gs': sems, 'gr': sems, 'gl': dma((1,))})


class Exchange:
    def __init__(self, t, n, src, dst, sems):
        self.t, self.n, self.src, self.dst = t, n, src, dst
        self.ss, self.rs, self.ls = sems

    def send(self, k):
        to = lax.rem(self.t.me + k, self.n)
        return remote(self.src(to), self.dst.at[self.t.me], self.ss.at[k], self.rs.at[k], to)

    def start(self):
        def body(k, _):
            self.send(k).start()
            return 0

        self.own = pltpu.make_async_copy(self.src(self.t.me), self.dst.at[self.t.me], self.ls.at[0])
        self.own.start()
        lax.fori_loop(1, self.n, body, 0)

    def finish(self):
        def body(k, _):
            fr = lax.rem(self.t.me - k + self.n, self.n)
            remote(self.src(fr), self.dst.at[fr], self.ss.at[k], self.rs.at[k], fr).wait_recv()
            self.send(k).wait_send()
            return 0

        lax.fori_loop(1, self.n, body, 0)
        self.own.wait()


class Tables:
    def __init__(self, t, n, r):
        self.t, self.r = t, r
        flat = lambda i: r.g.at[i // (2 * t.nx), lax.rem(i // 2, t.nx), lax.rem(i, 2)]
        self.experts = Exchange(t, n, flat, r.g_recv, (r.ts, r.tr, r.tl))

    def start(self):
        t, r = self.t, self.r
        by_x, by_y = r.lines.at[0], r.lines.at[1]
        self.own = [pltpu.make_async_copy(r.g.at[t.y], by_x.at[t.y], r.tl.at[1]),
                    pltpu.make_async_copy(r.g.at[:, t.x], by_y.at[t.x], r.tl.at[2])]
        for cp in self.own:
            cp.start()
        self.lines = []
        for d in range(1, RING):
            y, x = lax.rem(t.y + d, RING), lax.rem(t.x + d, RING)
            fy, fx = lax.rem(t.y + RING - d, RING), lax.rem(t.x + RING - d, RING)
            for h, src, dst, me, fr in ((1, r.g.at[y], by_x, t.y, fy), (0, r.g.at[:, x], by_y, t.x, fx)):
                self.lines += [remote(src, dst.at[i], r.us.at[h, d], r.ur.at[h, d], t.at(*hops(h, d))) for i in (me, fr)]
        for cp in self.lines[::2]:
            cp.start()
        self.experts.start()

    def finish(self):
        self.experts.finish()
        for cp, arrival in zip(self.lines[::2], self.lines[1::2]):
            arrival.wait_recv()
            cp.wait_send()
        for cp in self.own:
            cp.wait()


CHUNK = 512


class Shared:
    def __init__(self, r):
        self.r = r
        self.copies = [pltpu.make_async_copy(a, b, r.wl.at[i])
                       for i, (a, b) in enumerate(((r.ws1, r.v1), (r.ws3, r.v3), (r.ws2, r.v2)))]
        for cp in self.copies:
            cp.start()

    def ready(self):
        for cp in self.copies:
            cp.wait()

    def loop(self, out, step):
        out[...] = jnp.zeros_like(out)

        def body(i, _):
            out[...] += step(pl.ds(pl.multiple_of(i * CHUNK, CHUNK), CHUNK))
            return 0

        lax.fori_loop(0, self.r.v1.shape[1] // CHUNK, body, 0)

    def forward(self, x_t, out):
        r, x = self.r, x_t.T

        def step(at):
            return mm_nt(r.v2[:, at], hidden_of(mm(x, r.v1[:, at]), mm(x, r.v3[:, at]))[1])

        self.loop(out, step)

    def backward(self, x_t, dy_t, out):
        r, x, dy = self.r, x_t.T, dy_t.T

        def step(at):
            a1, a3 = mm(x, r.v1[:, at]), mm(x, r.v3[:, at])
            da1, da3 = swiglu_grads(a1, a3, mm(dy, r.v2[:, at]))
            return mm_nt(r.v1[:, at], da1) + mm_nt(r.v3[:, at], da3)

        self.loop(out, step)


def shared_parts(ws1, ws3, ws2):
    buf = VMEM(ws1.shape, BF16)
    return ({'ws1': (ws1, HBM), 'ws3': (ws3, HBM), 'ws2': (ws2.T, HBM)},
            {'v1': buf, 'v3': buf, 'v2': buf, 'wl': dma((3,))})


def gather_first(x_t, g, n, cid):
    tokens = g.shape[2]
    side = math.isqrt(n // 2)
    by = (side, side, 2, 8, tokens)
    ins, outs, scratch = gather_parts(x_t, n)
    table, lines = dma((n,)), dma((2, RING))

    def body(r):
        t = Torus(n)
        barrier_all(n)
        gather, tables = Gather(t, r, x_t.shape[0]), Tables(t, n, r)
        gather.start()
        tables.start()
        gather.run()
        tables.finish()
        gather.finish()

    res = run_kernel(body, cid, {**ins, 'g': (g.reshape(by), HBM)},
                     {**outs, 'g_recv': ((n, 8, tokens), F32, HBM), 'lines': ((2,) + by, F32, HBM)},
                     {**scratch, 'ts': table, 'tr': table, 'tl': dma((3,)), 'us': lines, 'ur': lines})
    return res.gathered, res.g_recv, res.lines.reshape(2, side, 2 * side, 8, tokens)


def gather_block(block, n, cid):
    ins, outs, scratch = gather_parts(block, n)

    def body(r):
        t = Torus(n)
        barrier_some(around(t))
        gather = Gather(t, r, block.shape[0])
        gather.start()
        gather.run()
        gather.finish()

    return run_kernel(body, cid, ins, outs, scratch).gathered


class Late:
    def __init__(self, r, capacity):
        self.r, self.capacity = r, capacity
        self.copies = [pltpu.make_async_copy(a, b, r.el.at[i]) for i, (a, b) in
                       enumerate(((r.rows, r.rv), (r.w1, r.u1), (r.w3, r.u3), (r.w2, r.u2)))]
        for cp in self.copies:
            cp.start()

    def run(self):
        r = self.r
        width = 2 * self.capacity
        for cp in self.copies:
            cp.wait()
        for e in PAIR:
            r.u2t[e] = r.u2[e].T

        def body(i, _):
            o = []
            for e in PAIR:
                rows = r.rv[e, :, pl.ds(pl.multiple_of(i * 4 * width, 4 * width), 4 * width)]
                o.append(mm(r.u2t[e], hidden_of(mm(r.u1[e], rows), mm(r.u3[e], rows))[1]))
            for p in range(4):
                halves = swap_halves(*[v[:, p * width:(p + 1) * width] for v in o])
                for k in PAIR:
                    r.ov[8 * i + 2 * p + k] = halves[k].astype(BF16)
            return 0

        lax.fori_loop(0, r.rv.shape[2] // (4 * width), body, 0)
        self.out = pltpu.make_async_copy(r.ov, r.o, r.el.at[0])
        self.out.start()

    def finish(self):
        self.out.wait()


def late_parts(rows, weights, capacity, n):
    d, w = rows.shape[1], VMEM(weights[0].shape, BF16)
    sends = (n, d, 2 * capacity)
    return ({'rows': (rows, HBM), **{k: (v, HBM) for k, v in zip(('w1', 'w3', 'w2'), weights)}},
            {'o': (sends, BF16, HBM)},
            {'rv': VMEM(rows.shape, BF16), 'u1': w, 'u3': w, 'u2': w, 'u2t': VMEM((2, d, w.shape[1]), BF16),
             'ov': VMEM(sends, BF16), 'el': dma((4,))})


def mm(a, b):
    return jnp.dot(a, b, preferred_element_type=F32)


def mm_nt(a, b):
    return lax.dot_general(a, b, NT, preferred_element_type=F32)


def slots_of(gates):
    tokens = gates.shape[1]
    before = (lax.broadcasted_iota(jnp.int32, (tokens, tokens), 0)
              < lax.broadcasted_iota(jnp.int32, (tokens, tokens), 1))
    member = gates > 0.0
    count = mm(jnp.where(member, 1.0, 0.0).astype(BF16), jnp.where(before, 1.0, 0.0).astype(BF16))
    return jnp.where(member, count, -1.0)


def pick(slot_rows, capacity):
    tokens = slot_rows[0].shape[1]
    want = lax.broadcasted_iota(jnp.int32, (capacity, tokens), 0).astype(F32)
    return jnp.concatenate([jnp.where(s == want, 1.0, 0.0) for s in slot_rows], axis=0)


def split3(v):
    a = v.astype(BF16).astype(F32)
    r = v - a
    b = r.astype(BF16).astype(F32)
    return a, b, r - b


def swap_halves(first, second):
    low = lax.broadcasted_iota(jnp.int32, first.shape, 1) < first.shape[1] // 2
    return jnp.where(low, first, second), jnp.where(low, second, first)


def hidden_of(a1, a3):
    sigma = jax.nn.sigmoid(a1)
    return sigma, (a1 * sigma * a3).astype(BF16)


def source_hot(slots, s, row, capacity):
    return pick([slots[8 * s + row:8 * s + row + 1], slots[8 * s + row + 1:8 * s + row + 2]], capacity).astype(BF16)


def pair_rows(block, p, slots, row, capacity):
    return swap_halves(*[mm_nt(block[s], source_hot(slots, s, row, capacity)) for s in (2 * p, 2 * p + 1)])


def forward_kernel(row, capacity, x_ref, g_ref, w1_ref, w3_ref, w2_ref, o_ref, w2t):
    sources = x_ref.shape[0]

    @pl.when(pl.program_id(0) == 0)
    def _():
        for e in PAIR:
            w2t[e] = w2_ref[e].T

    slots = slots_of(g_ref[...].reshape(sources * 8, -1))
    pairs = [pair_rows(x_ref, p, slots, row, capacity) for p in range(sources // 2)]
    o = []
    for e in PAIR:
        rows = jnp.concatenate([pr[e].astype(BF16) for pr in pairs], axis=1)
        hidden = hidden_of(mm(w1_ref[e], rows), mm(w3_ref[e], rows))[1]
        o.append(mm(w2t[e], hidden))
    width = 2 * capacity
    for p in range(sources // 2):
        a, b = swap_halves(o[0][:, p * width:(p + 1) * width], o[1][:, p * width:(p + 1) * width])
        o_ref[2 * p] = a.astype(BF16)
        o_ref[2 * p + 1] = b.astype(BF16)


def backward_kernel(row, capacity, keep, x_ref, dy_ref, g_ref, w1_ref, w3_ref, w2_ref,
                    dw1_ref, dw3_ref, dw2_ref, du_ref, gg_ref, *rest):
    w1n, w3n = rest[-2:]
    sources = dy_ref.shape[0]

    @pl.when(pl.program_id(0) == 0)
    def _():
        for ref in (dw1_ref, dw3_ref, dw2_ref):
            ref[...] = jnp.zeros_like(ref)
        for e in PAIR:
            w1n[e] = w1_ref[e].T
            w3n[e] = w3_ref[e].T

    d, tokens = dy_ref.shape[1:]
    width = 2 * capacity
    slots = slots_of(g_ref[...].reshape(sources * 8, -1))
    low = lax.broadcasted_iota(jnp.int32, (1, width), 1) < capacity
    hots, xp, dyp, gp = [], [], [], []
    for p in range(sources // 2):
        raw, gates, picked = [], [], []
        for s in (2 * p, 2 * p + 1):
            hot = source_hot(slots, s, row, capacity)
            hots.append(hot)
            picked.append(mm_nt(x_ref[s], hot))
            parts = split3(g_ref[s])
            extra = jnp.concatenate(list(parts) + [jnp.zeros_like(parts[0])], axis=0).astype(BF16)
            r = mm_nt(jnp.concatenate([dy_ref[s], extra], axis=0), hot)
            raw.append(r[:d])
            both = [r[d + i:d + i + 1] + r[d + 8 + i:d + 9 + i] + r[d + 16 + i:d + 17 + i] for i in (row, row + 1)]
            gates.append(jnp.where(low, *both))
        xp.append(swap_halves(*picked))
        dyp.append(swap_halves(*raw))
        gp.append(swap_halves(*gates))
    du, gg = [], []
    for e in PAIR:
        rows = jnp.concatenate([pr[e].astype(BF16) for pr in xp], axis=1)
        if keep:
            rest[0][e] = rows
        dy = jnp.concatenate([pr[e] for pr in dyp], axis=1)
        gate = jnp.concatenate([pr[e] for pr in gp], axis=1)
        a1, a3 = mm(w1_ref[e], rows), mm(w3_ref[e], rows)
        sigma, hidden = hidden_of(a1, a3)
        p32 = mm(w2_ref[e], dy.astype(BF16))
        gg.append(jnp.sum(hidden.astype(F32) * p32, axis=0, keepdims=True))
        dw2_ref[e] += mm_nt(hidden, (gate * dy).astype(BF16))
        q = gate * p32
        da1 = (q * a3 * sigma * (1.0 + a1 * (1.0 - sigma))).astype(BF16)
        da3 = (q * a1 * sigma).astype(BF16)
        dw1_ref[e] += mm_nt(da1, rows)
        dw3_ref[e] += mm_nt(da3, rows)
        du.append(mm(w1n[e], da1) + mm(w3n[e], da3))
    for p in range(sources // 2):
        at = slice(p * width, (p + 1) * width)
        for s, v in zip((2 * p, 2 * p + 1), swap_halves(du[0][:, at], du[1][:, at])):
            du_ref[s] = v.astype(BF16)
        for s, v in zip((2 * p, 2 * p + 1), swap_halves(gg[0][:, at], gg[1][:, at])):
            wide = jnp.broadcast_to(v, (8, width))
            expert = lax.broadcasted_iota(jnp.int32, (8, width), 0)
            block = lax.broadcasted_iota(jnp.int32, (8, width), 1) // capacity
            own = block == (expert if s % 2 == 0 else 1 - expert)
            parts = split3(jnp.where(own, wide, 0.0))
            res = mm(jnp.concatenate(list(parts) + [jnp.zeros_like(parts[0])], axis=0).astype(BF16), hots[s])
            gg_ref[s] = (res[:8] + res[8:16] + res[16:24])[:gg_ref.shape[1]]


SOURCES = 8


def whole(a):
    return pl.BlockSpec(a.shape, lambda i: (0,) * a.ndim)


def experts_forward(xg, gr, w1, w3, w2, row, capacity):
    n, tokens, d = xg.shape[0], xg.shape[2], w1.shape[2]
    grouped = lambda i: (i, 0, 0)
    return pl.pallas_call(
        functools.partial(forward_kernel, row, capacity),
        grid=(n // SOURCES,),
        out_shape=jax.ShapeDtypeStruct((n, d, 2 * capacity), BF16),
        out_specs=pl.BlockSpec((SOURCES, d, 2 * capacity), grouped),
        in_specs=[pl.BlockSpec((SOURCES, d, tokens), grouped), pl.BlockSpec((SOURCES, 8, tokens), grouped),
                  whole(w1), whole(w3), whole(w2)],
        scratch_shapes=[pltpu.VMEM((2, d, w2.shape[1]), BF16)],
        compiler_params=pltpu.CompilerParams(vmem_limit_bytes=VMEM_LIMIT),
    )(xg, gr, w1, w3, w2)


def experts_backward(both, gr, w1, w3, w2, row, capacity, keep):
    n, tokens, d = both.shape[0], both.shape[2], w1.shape[2]
    f = w2.shape[1]
    grouped = lambda i: (i, 0, 0)
    grads = [jax.ShapeDtypeStruct((2, f, d), F32)] * 3
    kept = [jax.ShapeDtypeStruct((2, d, n * capacity), BF16)] if keep else []
    return pl.pallas_call(
        functools.partial(backward_kernel, row, capacity, keep),
        grid=(n // SOURCES,),
        out_shape=grads + [jax.ShapeDtypeStruct((n, d, 2 * capacity), BF16),
                           jax.ShapeDtypeStruct((n, 2, tokens), F32)] + kept,
        out_specs=[whole(g) for g in grads] + [pl.BlockSpec((SOURCES, d, 2 * capacity), grouped),
                                               pl.BlockSpec((SOURCES, 2, tokens), grouped)]
        + [pl.BlockSpec((2, d, SOURCES * capacity), lambda i: (0, 0, i)) for _ in kept],
        in_specs=[pl.BlockSpec((SOURCES, d, tokens), grouped), pl.BlockSpec((SOURCES, d, tokens), lambda i: (i, 1, 0)),
                  pl.BlockSpec((SOURCES, 8, tokens), grouped), whole(w1), whole(w3), whole(w2)],
        scratch_shapes=[pltpu.VMEM((2, d, f), BF16)] * 2,
        compiler_params=pltpu.CompilerParams(vmem_limit_bytes=VMEM_LIMIT),
    )(both, both, gr, w1, w3, w2)


FAR_TO_NEAR = (2, 1, -1, 0)
RETURN_SCRATCH = ('recv', 'part', 'fin', 'ss', 'rs', 'ss2', 'rs2', 'ls', 'slots', 'acc')


class Return:
    def __init__(self, torus, r, name, row, capacity, gated):
        self.t, self.row, self.capacity, self.gated = torus, row, capacity, gated
        for field in ('src', 'out', *RETURN_SCRATCH):
            setattr(self, field, getattr(r, name + field))
        self.tables = r.lines
        self.half = self.src.shape[3] // 2
        self.sent = []

    def pos(self, h):
        return (self.t.x, self.t.y) if h == 0 else (self.t.y, self.t.x)

    def source(self, h, p, q, core):
        rows = pl.ds(h * self.half, self.half)
        a, b = (q, p) if h == 0 else (p, q)
        return self.src.at[a, b, core, rows, :]

    def send(self, src, dst, ssem, rsem, to):
        cp = remote(src, dst, ssem, rsem, to)
        cp.start()
        self.sent.append(cp)

    def sends(self, j):
        c = self.t.c
        for h in PAIR:
            p, q0 = self.pos(h)
            q = lax.rem(q0 + FAR_TO_NEAR[j] + RING, RING)
            dst = self.recv.at[h, j, p * 2 + c]
            ss, rs = self.ss.at[h, j], self.rs.at[h, j]
            for i, d in enumerate((2, 1, -1)):
                for core in PAIR:
                    self.send(self.source(h, lax.rem(p + d + RING, RING), q, core), dst, ss.at[2 * i + core],
                              rs.at[2 * i + c], self.t.at(*hops(h, d), core))
            self.send(self.source(h, p, q, 1 - c), dst, ss.at[6], rs.at[6], self.t.at(0, 0, 1 - c))
            pltpu.make_async_copy(self.source(h, p, q, c), dst, self.ls.at[h, j]).start()

    def arrive(self, dst, sem):
        remote(dst, dst, sem, sem, self.t.at(1, 0)).wait_recv()

    def arrivals(self, j):
        for h in PAIR:
            dst = self.recv.at[h, j, 0]
            for slot in range(7):
                self.arrive(dst, self.rs.at[h, j, slot])
            pltpu.make_async_copy(dst, dst, self.ls.at[h, j]).wait()

    def combine(self, j):
        def half(h, _):
            q0 = jnp.where(h == 0, self.t.y, self.t.x)
            gates = self.tables.at[h, lax.rem(q0 + FAR_TO_NEAR[j] + RING, RING)]
            senders, rows, tokens = gates.shape
            self.slots[...] = slots_of(gates[...].reshape(senders * rows, tokens)).reshape(gates.shape)
            self.acc[...] = jnp.zeros_like(self.acc)

            def body(m, _):
                ks = [2 * m + i for i in PAIR]
                lhs = jnp.concatenate([self.recv[h, j, k] for k in ks], axis=1)
                pairs = [(k, pl.ds(self.row + e, 1)) for k in ks for e in PAIR]
                hot = pick([self.slots[at] for at in pairs], self.capacity)
                weights = [hot]
                if self.gated:
                    parts = [split3(gates[at]) for at in pairs]
                    weights = [hot * jnp.concatenate([jnp.broadcast_to(g, (self.capacity, tokens)) for g in part], axis=0)
                               for part in zip(*parts)]
                self.acc[...] += sum(mm(lhs, w.astype(BF16)) for w in weights)
                return 0

            lax.fori_loop(0, senders // 2, body, 0)
            self.part[h, j] = self.acc[...]
            return 0

        lax.fori_loop(0, 2, half, 0)

    def round(self, j):
        self.combine(j)
        if j < RING - 1:
            for h in PAIR:
                self.send(self.part.at[h, j], self.fin.at[h, j], self.ss2.at[h, j], self.rs2.at[h, j],
                          self.t.at(*hops(h, 0, FAR_TO_NEAR[j])))

    def finish(self):
        for h in PAIR:
            for j in range(RING - 1):
                self.arrive(self.fin.at[h, j], self.rs2.at[h, j])
            at = slice(h * self.half, (h + 1) * self.half)
            self.out[at, :] = self.part[h, RING - 1] + self.fin[h, 0] + self.fin[h, 1] + self.fin[h, 2]
        for cp in self.sent:
            cp.wait_send()


def return_parts(name, rows, tokens, n):
    d, width = rows.shape[1:]
    side = math.isqrt(n // 2)
    half = d // 2
    first, second = dma((2, RING, 7)), dma((2, RING))
    shapes = (VMEM((2, RING, 2 * RING, half, width), BF16), VMEM((2, RING, half, tokens), F32),
              VMEM((2, RING - 1, half, tokens), F32), first, first, second, second, second,
              VMEM((2 * RING, 8, tokens), F32), VMEM((half, tokens), F32))
    return ({name + 'src': (rows.reshape(side, side, 2, d, width), HBM)},
            {**{name + f: shape for f, shape in zip(RETURN_SCRATCH, shapes)}, name + 'out': VMEM((d, tokens), F32)})


def drive(todo, work):
    for r in todo:
        for j in range(RING):
            r.sends(j)
    work()
    for r in todo:
        for j in range(RING):
            r.arrivals(j)
            r.round(j)
    for r in todo:
        r.finish()


def gg_parts(gg, n):
    sems = dma((n,))
    return {'gg': (gg, HBM)}, {'dg': (gg.shape, F32, HBM)}, {'qs': sems, 'qr': sems, 'ql': dma((1,))}


def return_first(o, lines, x_t, dy_t, weights, row, capacity, n, cid):
    d, tokens = x_t.shape
    ins, scratch = return_parts('o', o, tokens, n)
    w_ins, w_scratch = shared_parts(*weights)

    def body(r):
        t = Torus(n)
        shared = Shared(r)
        barrier_some(lines_of(t))
        job = Return(t, r, 'o', row, capacity, True)

        def work():
            shared.ready()
            shared.forward(r.x[...], r.s)

        drive([job], work)
        r.block[:d] = (r.x[...].astype(F32) + r.s[...] + job.out[...]).astype(BF16)
        r.block[d:] = r.dy[...]

    return run_kernel(body, cid, {**ins, **w_ins, 'lines': (lines, VMEM), 'x': (x_t, VMEM), 'dy': (dy_t, VMEM)},
                      {'block': ((2 * d, tokens), BF16, VMEM)},
                      {**scratch, **w_scratch, 's': VMEM((d, tokens), F32)}).block


def return_second(du, gg, lines, block, x_t, rows, experts, weights, row, capacity, n, cid):
    d, tokens = x_t.shape
    ins, scratch = return_parts('u', du, tokens, n)
    g_ins, g_outs, g_scratch = gg_parts(gg, n)
    w_ins, w_scratch = shared_parts(*weights)
    l_ins, l_outs, l_scratch = late_parts(rows, experts, capacity, n)

    def body(r):
        t = Torus(n)
        shared, late = Shared(r), Late(r, capacity)
        barrier_all(n)
        back = Exchange(t, n, lambda i: r.gg.at[i], r.dg, (r.qs, r.qr, r.ql))
        back.start()
        u = Return(t, r, 'u', row, capacity, False)

        def work():
            late.run()
            shared.ready()
            shared.backward(r.x1dy[:d], r.x1dy[d:], r.ds)
            shared.forward(r.x1dy[:d], r.s)

        drive([u], work)
        r.block[:d] = r.x[...]
        r.block[d:] = (r.x1dy[d:].astype(F32) + r.ds[...] + u.out[...]).astype(BF16)
        back.finish()
        late.finish()

    res = run_kernel(body, cid, {**ins, **g_ins, **w_ins, **l_ins, 'lines': (lines, VMEM), 'x1dy': (block, VMEM),
                                 'x': (x_t, VMEM)},
                     {**g_outs, **l_outs, 'block': (block.shape, BF16, VMEM), 's': ((d, tokens), F32, VMEM)},
                     {**scratch, **g_scratch, **w_scratch, **l_scratch, 'ds': VMEM((d, tokens), F32)})
    return res.block, res.dg, res.o, res.s


def return_third(du, o, gg, lines, block, x1dy, s, weights, rows_of, capacity, n, cid):
    d, tokens = s.shape
    u_ins, u_scratch = return_parts('u', du, tokens, n)
    o_ins, o_scratch = return_parts('o', o, tokens, n)
    g_ins, g_outs, g_scratch = gg_parts(gg, n)
    w_ins, w_scratch = shared_parts(*weights)

    def body(r):
        t = Torus(n)
        shared = Shared(r)
        barrier_all(n)
        back = Exchange(t, n, lambda i: r.gg.at[i], r.dg, (r.qs, r.qr, r.ql))
        back.start()
        u = Return(t, r, 'u', rows_of[0], capacity, False)
        o = Return(t, r, 'o', rows_of[1], capacity, True)

        def work():
            shared.ready()
            shared.backward(r.xdy[:d], r.xdy[d:], r.ds)

        drive([o, u], work)
        r.last[...] = (r.x1dy[:d].astype(F32) + r.s[...] + o.out[...]).astype(BF16)
        r.dx[...] = (r.xdy[d:].astype(F32) + r.ds[...] + u.out[...]).astype(BF16)
        back.finish()

    res = run_kernel(body, cid, {**u_ins, **o_ins, **g_ins, **w_ins, 'lines': (lines, VMEM),
                                 'xdy': (block, VMEM), 'x1dy': (x1dy, VMEM), 's': (s, VMEM)},
                     {**g_outs, 'dx': ((d, tokens), BF16, VMEM), 'last': ((d, tokens), BF16, VMEM)},
                     {**u_scratch, **o_scratch, **g_scratch, **w_scratch, 'ds': VMEM((d, tokens), F32)})
    return res.dx, res.last, res.dg


def swiglu_grads(pre_gate, pre_up, d_hidden):
    sigma = jax.nn.sigmoid(pre_gate)
    d_gate = d_hidden * pre_up * sigma * (1.0 + pre_gate * (1.0 - sigma))
    d_up = d_hidden * pre_gate * sigma
    return d_gate.astype(BF16), d_up.astype(BF16)


def gate_table(idx, gate, n_experts):
    ids = jnp.arange(n_experts, dtype=idx.dtype)[:, None, None]
    return jnp.sum(jnp.where(idx.T[None] == ids, gate.T[None], 0.0), axis=1)


def pair_gates(dg, idx):
    ids = jnp.arange(dg.shape[0], dtype=idx.dtype)[:, None, None]
    return jnp.sum(jnp.where(idx.T[None] == ids, dg[:, None, :], 0.0), axis=0).T


def solution(mesh):
    n = mesh.shape['ep']
    token_spec = P(('dp', 'ep'), None)
    expert_spec = P('ep', None, None)
    shared_spec = P(None, None)
    grad_spec = P(('dp', 'ep'), None, None)
    layer_specs = (expert_spec,) * 3 + (shared_spec,) * 3

    def device_step(x_in, d_out, idx_a, gate_a, idx_b, gate_b,
                    w1_a, w3_a, w2_a, ws1_a, ws3_a, ws2_a,
                    w1_b, w3_b, w2_b, ws1_b, ws3_b, ws2_b):
        tokens, top_k = idx_a.shape
        n_experts = w1_a.shape[0] * n
        capacity = top_k * ((2 * tokens + n_experts - 1) // n_experts)

        flip = lambda w: jnp.swapaxes(w, 1, 2)
        w1_a, w3_a, w1_b, w3_b = flip(w1_a), flip(w3_a), flip(w1_b), flip(w3_b)

        odd = lax.rem(lax.axis_index('ep'), 2) == 1
        tables = [gate_table(i, g, n_experts).reshape(n, 2, tokens) for i, g in ((idx_a, gate_a), (idx_b, gate_b))]
        tables = [jnp.where(odd, t[:, ::-1], t) for t in tables]
        g_own = jnp.concatenate(tables + [jnp.zeros((n, 4, tokens), F32)], axis=1)

        x_t, dy_t = x_in.T, d_out.T
        shared_a, shared_b = (ws1_a, ws3_a, ws2_a), (ws1_b, ws3_b, ws2_b)
        xg, g_recv, lines = gather_first(x_t, g_own, n, 0)
        o_a = experts_forward(xg, g_recv, w1_a, w3_a, w2_a, 0, capacity)
        x1dy = return_first(o_a, lines, x_t, dy_t, shared_a, 0, capacity, n, 1)

        both = gather_block(x1dy, n, 2)
        experts_b = (w1_b, w3_b, w2_b)
        dw1_b, dw3_b, dw2_b, du_b, gg_b, rows_b = experts_backward(both, g_recv, *experts_b, 2, capacity, True)
        block, dg_b, o_b, s_b = return_second(du_b, gg_b, lines, x1dy, x_t, rows_b, experts_b, shared_b, 2, capacity, n, 3)

        both = gather_block(block, n, 4)
        dw1_a, dw3_a, dw2_a, du_a, gg_a = experts_backward(both, g_recv, w1_a, w3_a, w2_a, 0, capacity, False)
        d_first, x_last, dg_a = return_third(du_a, o_b, gg_a, lines, block, x1dy, s_b, shared_a, (0, 2), capacity, n, 5)
        x_last, d_first = x_last.T, d_first.T

        return (x_last, d_first, flip(dw1_a), flip(dw3_a), dw2_a, flip(dw1_b), flip(dw3_b), dw2_b,
                pair_gates(dg_a.reshape(n_experts, tokens), idx_a), pair_gates(dg_b.reshape(n_experts, tokens), idx_b))

    in_specs = (token_spec,) * 6 + layer_specs + layer_specs
    out_specs = (token_spec, token_spec) + (grad_spec,) * 6 + (token_spec, token_spec)
    return jax.shard_map(device_step, mesh=mesh, in_specs=in_specs, out_specs=out_specs, check_vma=False)
```

```python
import functools
import math
from types import SimpleNamespace

import jax
import jax.numpy as jnp
from jax import lax
from jax.experimental import pallas as pl
from jax.experimental.pallas import tpu as pltpu
from jax.sharding import PartitionSpec as P

MESH = pl.DeviceIdType.MESH
F32, BF16 = jnp.float32, jnp.bfloat16
NT = (((1,), (1,)), ((), ()))
VMEM_LIMIT = 62914560
PAIR = (0, 1)
SIDES = (1, -1)


def dev(i):
    return {'ep': i}


class Torus:
    def __init__(self, n):
        self.nx = math.isqrt(n // 2)
        self.ny = n // 2 // self.nx
        self.me = lax.axis_index('ep')
        self.c = lax.rem(self.me, 2)
        chip = self.me // 2
        self.x, self.y = lax.rem(chip, self.nx), chip // self.nx

    def at(self, dx, dy, c=None):
        x = lax.rem(self.x + dx + self.nx, self.nx)
        y = lax.rem(self.y + dy + self.ny, self.ny)
        return (y * self.nx + x) * 2 + (self.c if c is None else c)


def barrier_all(n):
    me = lax.axis_index('ep')
    b = pltpu.get_barrier_semaphore()

    def body(k, _):
        pl.semaphore_signal(b, inc=1, device_id=dev(lax.rem(me + k, n)), device_id_type=MESH)
        return 0

    lax.fori_loop(1, n, body, 0)
    pl.semaphore_wait(b, n - 1)


def remote(src, dst, ssem, rsem, to):
    return pltpu.make_async_remote_copy(src_ref=src, dst_ref=dst, send_sem=ssem, recv_sem=rsem,
                                        device_id=dev(to), device_id_type=MESH)


def barrier_some(partners):
    b = pltpu.get_barrier_semaphore()
    for p in partners:
        pl.semaphore_signal(b, inc=1, device_id=dev(p), device_id_type=MESH)
    pl.semaphore_wait(b, len(partners))


def around(t):
    return [t.at(*hops(h, d)) for h in PAIR for d in SIDES] + [t.at(0, 0, 1 - t.c)]


def lines_of(t):
    return [t.at(*hops(h, d), c) for h in PAIR for d in (1, -1, 2) for c in PAIR] + [t.at(0, 0, 1 - t.c)]


def run_kernel(body, cid, ins, outs, scratch):
    names = [*ins, *outs, *scratch]

    def kernel(*refs):
        body(SimpleNamespace(**dict(zip(names, refs))))

    spec = lambda space: pl.BlockSpec(memory_space=space)
    res = pl.pallas_call(
        kernel,
        out_shape=[jax.ShapeDtypeStruct(shape, dtype) for shape, dtype, _ in outs.values()],
        in_specs=[spec(space) for _, space in ins.values()],
        out_specs=[spec(space) for _, _, space in outs.values()],
        scratch_shapes=list(scratch.values()),
        compiler_params=pltpu.CompilerParams(collective_id=cid, has_side_effects=True, vmem_limit_bytes=VMEM_LIMIT),
    )(*[array for array, _ in ins.values()])
    return SimpleNamespace(**dict(zip(outs, res)))


RING = 4
HBM, VMEM = pl.ANY, pltpu.VMEM
dma = pltpu.SemaphoreType.DMA


def hops(h, d, e=0):
    return (d, e) if h == 0 else (e, d)


class Gather:
    def __init__(self, torus, r, rows):
        self.t, self.block, self.out, self.ssem, self.rsem, self.lsem = torus, r.block, r.gathered, r.gs, r.gr, r.gl
        self.half, self.quarter = rows // 2, rows // 4
        self.count, self.sent, self.sibling, self.m = 0, [], [], {}

    def ref(self, off, r0, nr, core=None):
        return self.out.at[self.t.at(*off, core), pl.ds(r0, nr), :]

    def send(self, off, r0, nr, to):
        i = self.count
        self.count += 1
        ref = self.ref(off, r0, nr)
        src = self.block.at[pl.ds(r0, nr), :] if off == (0, 0) else ref
        cp = remote(src, ref, self.ssem.at[i], self.rsem.at[i], to)
        cp.start()
        self.sent.append(cp)
        return i

    def move(self, off, r0, nr, to):
        return self.send(off, r0, nr, self.t.at(*to)), nr

    def arrive(self, ref, i):
        remote(ref, ref, self.ssem.at[i], self.rsem.at[i], self.t.at(1, 0)).wait_recv()

    def wait(self, off, r0, mv):
        self.arrive(self.ref(off, r0, mv[1]), mv[0])

    def to_sibling(self, off, r0, nr):
        self.sibling.append((off, r0, nr, self.send(off, r0, nr, self.t.at(0, 0, 1 - self.t.c))))

    def start(self):
        m, half = self.m, self.half
        for h in PAIR:
            for d in SIDES:
                m[h, 'own', d] = self.move((0, 0), h * half, half, hops(h, d))
        for h in PAIR:
            for d in SIDES:
                m[h, 0, d] = self.move((0, 0), h * half, half, hops(h, 0, d))
        self.to_sibling((0, 0), 0, half * 2)
        self.own = pltpu.make_async_copy(self.block, self.out.at[self.t.me], self.lsem.at[0])
        self.own.start()

    def across(self, h, b):
        for k, e in enumerate(SIDES):
            off = hops(h, b, -e)
            self.wait(off, h * self.half, self.m[h, b, e])
            self.m[h, b, e, 'on'] = self.move(off, h * self.half + k * self.quarter, self.quarter, hops(h, 0, e))
            self.to_sibling(off, h * self.half, self.half)

    def spread(self, h, b):
        for e in SIDES:
            self.m[h, b, e] = self.move(hops(h, b), h * self.half, self.half, hops(h, 0, e))
        self.to_sibling(hops(h, b), h * self.half, self.half)

    def run(self, then=None):
        m, half, q = self.m, self.half, self.quarter
        for h in PAIR:
            for k, d in enumerate(SIDES):
                self.wait(hops(h, -d), h * half, m[h, 'own', d])
                m[h, 'on', d] = self.move(hops(h, -d), h * half + k * q, q, hops(h, d))
                self.spread(h, -d)
        if then:
            then()
        for h in PAIR:
            self.across(h, 0)
        for h in PAIR:
            for k, d in enumerate(SIDES):
                self.wait(hops(h, -2 * d), h * half + k * q, m[h, 'on', d])
            self.spread(h, 2)
        for b in (-1, 1, 2):
            for h in PAIR:
                self.across(h, b)
        for b in (0, -1, 1, 2):
            for h in PAIR:
                for k, e in enumerate(SIDES):
                    self.wait(hops(h, b, -2 * e), h * half + k * q, m[h, b, e, 'on'])
                self.to_sibling(hops(h, b, 2), h * half, half)

    def finish(self):
        for off, r0, nr, i in self.sibling:
            self.arrive(self.ref(off, r0, nr, 1 - self.t.c), i)
        for cp in self.sent:
            cp.wait_send()
        self.own.wait()


def gather_parts(block, n):
    sems = dma((80,))
    return ({'block': (block, HBM)}, {'gathered': ((n,) + block.shape, block.dtype, HBM)},
            {'gs': sems, 'gr': sems, 'gl': dma((1,))})


class Exchange:
    def __init__(self, t, n, src, dst, sems):
        self.t, self.n, self.src, self.dst = t, n, src, dst
        self.ss, self.rs, self.ls = sems

    def send(self, k):
        to = lax.rem(self.t.me + k, self.n)
        return remote(self.src(to), self.dst.at[self.t.me], self.ss.at[k], self.rs.at[k], to)

    def start(self):
        def body(k, _):
            self.send(k).start()
            return 0

        self.own = pltpu.make_async_copy(self.src(self.t.me), self.dst.at[self.t.me], self.ls.at[0])
        self.own.start()
        lax.fori_loop(1, self.n, body, 0)

    def finish(self):
        def body(k, _):
            fr = lax.rem(self.t.me - k + self.n, self.n)
            remote(self.src(fr), self.dst.at[fr], self.ss.at[k], self.rs.at[k], fr).wait_recv()
            self.send(k).wait_send()
            return 0

        lax.fori_loop(1, self.n, body, 0)
        self.own.wait()


class Tables:
    def __init__(self, t, n, r):
        self.t, self.r = t, r
        flat = lambda i: r.g.at[i // (2 * t.nx), lax.rem(i // 2, t.nx), lax.rem(i, 2)]
        self.experts = Exchange(t, n, flat, r.g_recv, (r.ts, r.tr, r.tl))

    def start(self):
        t, r = self.t, self.r
        by_x, by_y = r.lines.at[0], r.lines.at[1]
        self.own = [pltpu.make_async_copy(r.chips.at[t.y], by_x.at[t.y], r.tl.at[1]),
                    pltpu.make_async_copy(r.chips.at[:, t.x], by_y.at[t.x], r.tl.at[2])]
        for cp in self.own:
            cp.start()
        self.lines = []
        for d in range(1, RING):
            y, x = lax.rem(t.y + d, RING), lax.rem(t.x + d, RING)
            fy, fx = lax.rem(t.y + RING - d, RING), lax.rem(t.x + RING - d, RING)
            for h, src, dst, me, fr in ((1, r.chips.at[y], by_x, t.y, fy), (0, r.chips.at[:, x], by_y, t.x, fx)):
                self.lines += [remote(src, dst.at[i], r.us.at[h, d], r.ur.at[h, d], t.at(*hops(h, d))) for i in (me, fr)]
        for cp in self.lines[::2]:
            cp.start()
        self.experts.start()

    def finish(self):
        self.experts.finish()
        for cp, arrival in zip(self.lines[::2], self.lines[1::2]):
            arrival.wait_recv()
            cp.wait_send()
        for cp in self.own:
            cp.wait()


CHUNK = 512


class Shared:
    def __init__(self, r):
        self.r = r
        self.copies = [pltpu.make_async_copy(a, b, r.wl.at[i])
                       for i, (a, b) in enumerate(((r.ws1, r.v1), (r.ws3, r.v3), (r.ws2, r.v2)))]
        for cp in self.copies:
            cp.start()

    def ready(self):
        for cp in self.copies:
            cp.wait()

    def loop(self, out, step):
        out[...] = jnp.zeros_like(out)

        def body(i, _):
            out[...] += step(pl.ds(pl.multiple_of(i * CHUNK, CHUNK), CHUNK))
            return 0

        lax.fori_loop(0, self.r.v1.shape[1] // CHUNK, body, 0)

    def forward(self, x_t, out):
        r, x = self.r, x_t.T

        def step(at):
            return mm_nt(r.v2[:, at], hidden_of(mm(x, r.v1[:, at]), mm(x, r.v3[:, at]))[1])

        self.loop(out, step)

    def backward(self, x_t, dy_t, out):
        r, x, dy = self.r, x_t.T, dy_t.T

        def step(at):
            a1, a3 = mm(x, r.v1[:, at]), mm(x, r.v3[:, at])
            da1, da3 = swiglu_grads(a1, a3, mm(dy, r.v2[:, at]))
            return mm_nt(r.v1[:, at], da1) + mm_nt(r.v3[:, at], da3)

        self.loop(out, step)


def shared_parts(ws1, ws3, ws2):
    buf = VMEM(ws1.shape, BF16)
    return ({'ws1': (ws1, HBM), 'ws3': (ws3, HBM), 'ws2': (ws2.T, HBM)},
            {'v1': buf, 'v3': buf, 'v2': buf, 'wl': dma((3,))})


def gather_first(x_t, g, n, cid):
    tokens = g.shape[2]
    side = math.isqrt(n // 2)
    by = (side, side, 2, 8, tokens)
    chips = g[:, :4].reshape(side, side, 8, tokens)
    ins, outs, scratch = gather_parts(x_t, n)
    table, lines = dma((n,)), dma((2, RING))

    def body(r):
        t = Torus(n)
        barrier_all(n)
        gather, tables = Gather(t, r, x_t.shape[0]), Tables(t, n, r)
        gather.start()
        gather.run(tables.start)
        tables.finish()
        gather.finish()

    res = run_kernel(body, cid, {**ins, 'g': (g.reshape(by), HBM), 'chips': (chips, HBM)},
                     {**outs, 'g_recv': ((n, 8, tokens), F32, HBM), 'lines': ((2,) + chips.shape, F32, HBM)},
                     {**scratch, 'ts': table, 'tr': table, 'tl': dma((3,)), 'us': lines, 'ur': lines})
    return res.gathered, res.g_recv, res.lines


def gather_block(block, n, cid):
    ins, outs, scratch = gather_parts(block, n)

    def body(r):
        t = Torus(n)
        barrier_some(around(t))
        gather = Gather(t, r, block.shape[0])
        gather.start()
        gather.run()
        gather.finish()

    return run_kernel(body, cid, ins, outs, scratch).gathered


class Late:
    def __init__(self, r, capacity):
        self.r, self.capacity = r, capacity
        self.copies = [pltpu.make_async_copy(a, b, r.el.at[i]) for i, (a, b) in
                       enumerate(((r.rows, r.rv), (r.w1, r.u1), (r.w3, r.u3), (r.w2, r.u2)))]
        for cp in self.copies:
            cp.start()

    def run(self):
        r = self.r
        width = 2 * self.capacity
        for cp in self.copies:
            cp.wait()
        for e in PAIR:
            r.u2t[e] = r.u2[e].T

        def body(i, _):
            o = []
            for e in PAIR:
                rows = r.rv[e, :, pl.ds(pl.multiple_of(i * 4 * width, 4 * width), 4 * width)]
                o.append(mm(r.u2t[e], hidden_of(mm(r.u1[e], rows), mm(r.u3[e], rows))[1]))
            for p in range(4):
                halves = swap_halves(*[v[:, p * width:(p + 1) * width] for v in o])
                for k in PAIR:
                    r.ov[8 * i + 2 * p + k] = halves[k].astype(BF16)
            return 0

        lax.fori_loop(0, r.rv.shape[2] // (4 * width), body, 0)
        self.out = pltpu.make_async_copy(r.ov, r.o, r.el.at[0])
        self.out.start()

    def finish(self):
        self.out.wait()


def late_parts(rows, weights, capacity, n):
    d, w = rows.shape[1], VMEM(weights[0].shape, BF16)
    sends = (n, d, 2 * capacity)
    return ({'rows': (rows, HBM), **{k: (v, HBM) for k, v in zip(('w1', 'w3', 'w2'), weights)}},
            {'o': (sends, BF16, HBM)},
            {'rv': VMEM(rows.shape, BF16), 'u1': w, 'u3': w, 'u2': w, 'u2t': VMEM((2, d, w.shape[1]), BF16),
             'ov': VMEM(sends, BF16), 'el': dma((4,))})


def mm(a, b):
    return jnp.dot(a, b, preferred_element_type=F32)


def mm_nt(a, b):
    return lax.dot_general(a, b, NT, preferred_element_type=F32)


def slots_of(gates):
    tokens = gates.shape[1]
    before = (lax.broadcasted_iota(jnp.int32, (tokens, tokens), 0)
              < lax.broadcasted_iota(jnp.int32, (tokens, tokens), 1))
    member = gates > 0.0
    count = mm(jnp.where(member, 1.0, 0.0).astype(BF16), jnp.where(before, 1.0, 0.0).astype(BF16))
    return jnp.where(member, count, -1.0)


def pick(slot_rows, capacity):
    tokens = slot_rows[0].shape[1]
    want = lax.broadcasted_iota(jnp.int32, (capacity, tokens), 0).astype(F32)
    return jnp.concatenate([jnp.where(s == want, 1.0, 0.0) for s in slot_rows], axis=0)


def split3(v):
    a = v.astype(BF16).astype(F32)
    r = v - a
    b = r.astype(BF16).astype(F32)
    return a, b, r - b


def swap_halves(first, second):
    low = lax.broadcasted_iota(jnp.int32, first.shape, 1) < first.shape[1] // 2
    return jnp.where(low, first, second), jnp.where(low, second, first)


def hidden_of(a1, a3):
    sigma = jax.nn.sigmoid(a1)
    return sigma, (a1 * sigma * a3).astype(BF16)


def source_hot(slots, s, row, capacity):
    return pick([slots[8 * s + row:8 * s + row + 1], slots[8 * s + row + 1:8 * s + row + 2]], capacity).astype(BF16)


def pair_rows(block, p, slots, row, capacity):
    return swap_halves(*[mm_nt(block[s], source_hot(slots, s, row, capacity)) for s in (2 * p, 2 * p + 1)])


def forward_kernel(row, capacity, x_ref, g_ref, w1_ref, w3_ref, w2_ref, o_ref, w2t):
    sources = x_ref.shape[0]

    @pl.when(pl.program_id(0) == 0)
    def _():
        for e in PAIR:
            w2t[e] = w2_ref[e].T

    slots = slots_of(g_ref[...].reshape(sources * 8, -1))
    pairs = [pair_rows(x_ref, p, slots, row, capacity) for p in range(sources // 2)]
    o = []
    for e in PAIR:
        rows = jnp.concatenate([pr[e].astype(BF16) for pr in pairs], axis=1)
        hidden = hidden_of(mm(w1_ref[e], rows), mm(w3_ref[e], rows))[1]
        o.append(mm(w2t[e], hidden))
    width = 2 * capacity
    for p in range(sources // 2):
        a, b = swap_halves(o[0][:, p * width:(p + 1) * width], o[1][:, p * width:(p + 1) * width])
        o_ref[2 * p] = a.astype(BF16)
        o_ref[2 * p + 1] = b.astype(BF16)


def backward_kernel(row, capacity, keep, x_ref, dy_ref, g_ref, w1_ref, w3_ref, w2_ref,
                    dw1_ref, dw3_ref, dw2_ref, du_ref, gg_ref, *rest):
    w1n, w3n = rest[-2:]
    sources = dy_ref.shape[0]

    @pl.when(pl.program_id(0) == 0)
    def _():
        for ref in (dw1_ref, dw3_ref, dw2_ref):
            ref[...] = jnp.zeros_like(ref)
        for e in PAIR:
            w1n[e] = w1_ref[e].T
            w3n[e] = w3_ref[e].T

    d, tokens = dy_ref.shape[1:]
    width = 2 * capacity
    slots = slots_of(g_ref[...].reshape(sources * 8, -1))
    low = lax.broadcasted_iota(jnp.int32, (1, width), 1) < capacity
    hots, xp, dyp, gp = [], [], [], []
    for p in range(sources // 2):
        raw, gates, picked = [], [], []
        for s in (2 * p, 2 * p + 1):
            hot = source_hot(slots, s, row, capacity)
            hots.append(hot)
            picked.append(mm_nt(x_ref[s], hot))
            parts = split3(g_ref[s])
            extra = jnp.concatenate(list(parts) + [jnp.zeros_like(parts[0])], axis=0).astype(BF16)
            r = mm_nt(jnp.concatenate([dy_ref[s], extra], axis=0), hot)
            raw.append(r[:d])
            both = [r[d + i:d + i + 1] + r[d + 8 + i:d + 9 + i] + r[d + 16 + i:d + 17 + i] for i in (row, row + 1)]
            gates.append(jnp.where(low, *both))
        xp.append(swap_halves(*picked))
        dyp.append(swap_halves(*raw))
        gp.append(swap_halves(*gates))
    du, gg = [], []
    for e in PAIR:
        rows = jnp.concatenate([pr[e].astype(BF16) for pr in xp], axis=1)
        if keep:
            rest[0][e] = rows
        dy = jnp.concatenate([pr[e] for pr in dyp], axis=1)
        gate = jnp.concatenate([pr[e] for pr in gp], axis=1)
        a1, a3 = mm(w1_ref[e], rows), mm(w3_ref[e], rows)
        sigma, hidden = hidden_of(a1, a3)
        p32 = mm(w2_ref[e], dy.astype(BF16))
        gg.append(jnp.sum(hidden.astype(F32) * p32, axis=0, keepdims=True))
        dw2_ref[e] += mm_nt(hidden, (gate * dy).astype(BF16))
        q = gate * p32
        da1 = (q * a3 * sigma * (1.0 + a1 * (1.0 - sigma))).astype(BF16)
        da3 = (q * a1 * sigma).astype(BF16)
        dw1_ref[e] += mm_nt(da1, rows)
        dw3_ref[e] += mm_nt(da3, rows)
        du.append(mm(w1n[e], da1) + mm(w3n[e], da3))
    for p in range(sources // 2):
        at = slice(p * width, (p + 1) * width)
        for s, v in zip((2 * p, 2 * p + 1), swap_halves(du[0][:, at], du[1][:, at])):
            du_ref[s] = v.astype(BF16)
        for s, v in zip((2 * p, 2 * p + 1), swap_halves(gg[0][:, at], gg[1][:, at])):
            wide = jnp.broadcast_to(v, (8, width))
            expert = lax.broadcasted_iota(jnp.int32, (8, width), 0)
            block = lax.broadcasted_iota(jnp.int32, (8, width), 1) // capacity
            own = block == (expert if s % 2 == 0 else 1 - expert)
            parts = split3(jnp.where(own, wide, 0.0))
            res = mm(jnp.concatenate(list(parts) + [jnp.zeros_like(parts[0])], axis=0).astype(BF16), hots[s])
            gg_ref[s] = (res[:8] + res[8:16] + res[16:24])[:gg_ref.shape[1]]


SOURCES = 8


def whole(a):
    return pl.BlockSpec(a.shape, lambda i: (0,) * a.ndim)


def experts_forward(xg, gr, w1, w3, w2, row, capacity):
    n, tokens, d = xg.shape[0], xg.shape[2], w1.shape[2]
    grouped = lambda i: (i, 0, 0)
    return pl.pallas_call(
        functools.partial(forward_kernel, row, capacity),
        grid=(n // SOURCES,),
        out_shape=jax.ShapeDtypeStruct((n, d, 2 * capacity), BF16),
        out_specs=pl.BlockSpec((SOURCES, d, 2 * capacity), grouped),
        in_specs=[pl.BlockSpec((SOURCES, d, tokens), grouped), pl.BlockSpec((SOURCES, 8, tokens), grouped),
                  whole(w1), whole(w3), whole(w2)],
        scratch_shapes=[pltpu.VMEM((2, d, w2.shape[1]), BF16)],
        compiler_params=pltpu.CompilerParams(vmem_limit_bytes=VMEM_LIMIT),
    )(xg, gr, w1, w3, w2)


def experts_backward(both, gr, w1, w3, w2, row, capacity, keep):
    n, tokens, d = both.shape[0], both.shape[2], w1.shape[2]
    f = w2.shape[1]
    grouped = lambda i: (i, 0, 0)
    grads = [jax.ShapeDtypeStruct((2, f, d), F32)] * 3
    kept = [jax.ShapeDtypeStruct((2, d, n * capacity), BF16)] if keep else []
    return pl.pallas_call(
        functools.partial(backward_kernel, row, capacity, keep),
        grid=(n // SOURCES,),
        out_shape=grads + [jax.ShapeDtypeStruct((n, d, 2 * capacity), BF16),
                           jax.ShapeDtypeStruct((n, 2, tokens), F32)] + kept,
        out_specs=[whole(g) for g in grads] + [pl.BlockSpec((SOURCES, d, 2 * capacity), grouped),
                                               pl.BlockSpec((SOURCES, 2, tokens), grouped)]
        + [pl.BlockSpec((2, d, SOURCES * capacity), lambda i: (0, 0, i)) for _ in kept],
        in_specs=[pl.BlockSpec((SOURCES, d, tokens), grouped), pl.BlockSpec((SOURCES, d, tokens), lambda i: (i, 1, 0)),
                  pl.BlockSpec((SOURCES, 8, tokens), grouped), whole(w1), whole(w3), whole(w2)],
        scratch_shapes=[pltpu.VMEM((2, d, f), BF16)] * 2,
        compiler_params=pltpu.CompilerParams(vmem_limit_bytes=VMEM_LIMIT),
    )(both, both, gr, w1, w3, w2)


FAR_TO_NEAR = (2, 1, -1, 0)
RETURN_SCRATCH = ('recv', 'part', 'fin', 'ss', 'rs', 'ss2', 'rs2', 'ls', 'slots', 'acc')


class Return:
    def __init__(self, torus, r, name, row, capacity, gated):
        self.t, self.row, self.capacity, self.gated = torus, row, capacity, gated
        for field in ('src', 'out', *RETURN_SCRATCH):
            setattr(self, field, getattr(r, name + field))
        self.tables = r.lines
        self.half = self.src.shape[3] // 2
        self.sent = []

    def pos(self, h):
        return (self.t.x, self.t.y) if h == 0 else (self.t.y, self.t.x)

    def source(self, h, p, q, core):
        rows = pl.ds(h * self.half, self.half)
        a, b = (q, p) if h == 0 else (p, q)
        return self.src.at[a, b, core, rows, :]

    def send(self, src, dst, ssem, rsem, to):
        cp = remote(src, dst, ssem, rsem, to)
        cp.start()
        self.sent.append(cp)

    def sends(self, j):
        c = self.t.c
        for h in PAIR:
            p, q0 = self.pos(h)
            q = lax.rem(q0 + FAR_TO_NEAR[j] + RING, RING)
            dst = self.recv.at[h, j, p * 2 + c]
            ss, rs = self.ss.at[h, j], self.rs.at[h, j]
            for i, d in enumerate((2, 1, -1)):
                for core in PAIR:
                    self.send(self.source(h, lax.rem(p + d + RING, RING), q, core), dst, ss.at[2 * i + core],
                              rs.at[2 * i + c], self.t.at(*hops(h, d), core))
            self.send(self.source(h, p, q, 1 - c), dst, ss.at[6], rs.at[6], self.t.at(0, 0, 1 - c))
            pltpu.make_async_copy(self.source(h, p, q, c), dst, self.ls.at[h, j]).start()

    def arrive(self, dst, sem):
        remote(dst, dst, sem, sem, self.t.at(1, 0)).wait_recv()

    def arrivals(self, j):
        for h in PAIR:
            dst = self.recv.at[h, j, 0]
            for slot in range(7):
                self.arrive(dst, self.rs.at[h, j, slot])
            pltpu.make_async_copy(dst, dst, self.ls.at[h, j]).wait()

    def combine(self, j):
        def half(h, _):
            q0 = jnp.where(h == 0, self.t.y, self.t.x)
            gates = self.tables.at[h, lax.rem(q0 + FAR_TO_NEAR[j] + RING, RING)]
            chips, rows, tokens = gates.shape
            self.slots[...] = slots_of(gates[...].reshape(chips * rows, tokens)).reshape(gates.shape)
            self.acc[...] = jnp.zeros_like(self.acc)

            def body(m, _):
                ks = [2 * m + i for i in PAIR]
                lhs = jnp.concatenate([self.recv[h, j, k] for k in ks], axis=1)
                pairs = [(m, pl.ds(4 * i + self.row + e, 1)) for i in PAIR for e in PAIR]
                hot = pick([self.slots[at] for at in pairs], self.capacity)
                weights = [hot]
                if self.gated:
                    parts = [split3(gates[at]) for at in pairs]
                    weights = [hot * jnp.concatenate([jnp.broadcast_to(g, (self.capacity, tokens)) for g in part], axis=0)
                               for part in zip(*parts)]
                self.acc[...] += sum(mm(lhs, w.astype(BF16)) for w in weights)
                return 0

            lax.fori_loop(0, chips, body, 0)
            self.part[h, j] = self.acc[...]
            return 0

        lax.fori_loop(0, 2, half, 0)

    def round(self, j):
        self.combine(j)
        if j < RING - 1:
            for h in PAIR:
                self.send(self.part.at[h, j], self.fin.at[h, j], self.ss2.at[h, j], self.rs2.at[h, j],
                          self.t.at(*hops(h, 0, FAR_TO_NEAR[j])))

    def finish(self):
        for h in PAIR:
            for j in range(RING - 1):
                self.arrive(self.fin.at[h, j], self.rs2.at[h, j])
            at = slice(h * self.half, (h + 1) * self.half)
            self.out[at, :] = self.part[h, RING - 1] + self.fin[h, 0] + self.fin[h, 1] + self.fin[h, 2]
        for cp in self.sent:
            cp.wait_send()


def return_parts(name, rows, tokens, n):
    d, width = rows.shape[1:]
    side = math.isqrt(n // 2)
    half = d // 2
    first, second = dma((2, RING, 7)), dma((2, RING))
    shapes = (VMEM((2, RING, 2 * RING, half, width), BF16), VMEM((2, RING, half, tokens), F32),
              VMEM((2, RING - 1, half, tokens), F32), first, first, second, second, second,
              VMEM((RING, 8, tokens), F32), VMEM((half, tokens), F32))
    return ({name + 'src': (rows.reshape(side, side, 2, d, width), HBM)},
            {**{name + f: shape for f, shape in zip(RETURN_SCRATCH, shapes)}, name + 'out': VMEM((d, tokens), F32)})


def drive(todo, work):
    for r in todo:
        for j in range(RING):
            r.sends(j)
    work()
    for r in todo:
        for j in range(RING):
            r.arrivals(j)
            r.round(j)
    for r in todo:
        r.finish()


def gg_parts(gg, n):
    sems = dma((n,))
    return {'gg': (gg, HBM)}, {'dg': (gg.shape, F32, HBM)}, {'qs': sems, 'qr': sems, 'ql': dma((1,))}


def return_first(o, lines, x_t, dy_t, weights, row, capacity, n, cid):
    d, tokens = x_t.shape
    ins, scratch = return_parts('o', o, tokens, n)
    w_ins, w_scratch = shared_parts(*weights)

    def body(r):
        t = Torus(n)
        shared = Shared(r)
        barrier_some(lines_of(t))
        job = Return(t, r, 'o', row, capacity, True)

        def work():
            shared.ready()
            shared.forward(r.x[...], r.s)

        drive([job], work)
        r.block[:d] = (r.x[...].astype(F32) + r.s[...] + job.out[...]).astype(BF16)
        r.block[d:] = r.dy[...]

    return run_kernel(body, cid, {**ins, **w_ins, 'lines': (lines, VMEM), 'x': (x_t, VMEM), 'dy': (dy_t, VMEM)},
                      {'block': ((2 * d, tokens), BF16, VMEM)},
                      {**scratch, **w_scratch, 's': VMEM((d, tokens), F32)}).block


def return_second(du, gg, lines, block, x_t, rows, experts, weights, row, capacity, n, cid):
    d, tokens = x_t.shape
    ins, scratch = return_parts('u', du, tokens, n)
    g_ins, g_outs, g_scratch = gg_parts(gg, n)
    w_ins, w_scratch = shared_parts(*weights)
    l_ins, l_outs, l_scratch = late_parts(rows, experts, capacity, n)

    def body(r):
        t = Torus(n)
        shared, late = Shared(r), Late(r, capacity)
        barrier_all(n)
        back = Exchange(t, n, lambda i: r.gg.at[i], r.dg, (r.qs, r.qr, r.ql))
        back.start()
        u = Return(t, r, 'u', row, capacity, False)

        def work():
            late.run()
            shared.ready()
            shared.backward(r.x1dy[:d], r.x1dy[d:], r.ds)
            shared.forward(r.x1dy[:d], r.s)

        drive([u], work)
        r.block[:d] = r.x[...]
        r.block[d:] = (r.x1dy[d:].astype(F32) + r.ds[...] + u.out[...]).astype(BF16)
        back.finish()
        late.finish()

    res = run_kernel(body, cid, {**ins, **g_ins, **w_ins, **l_ins, 'lines': (lines, VMEM), 'x1dy': (block, VMEM),
                                 'x': (x_t, VMEM)},
                     {**g_outs, **l_outs, 'block': (block.shape, BF16, VMEM), 's': ((d, tokens), F32, VMEM)},
                     {**scratch, **g_scratch, **w_scratch, **l_scratch, 'ds': VMEM((d, tokens), F32)})
    return res.block, res.dg, res.o, res.s


def return_third(du, o, gg, lines, block, x1dy, s, weights, rows_of, capacity, n, cid):
    d, tokens = s.shape
    u_ins, u_scratch = return_parts('u', du, tokens, n)
    o_ins, o_scratch = return_parts('o', o, tokens, n)
    g_ins, g_outs, g_scratch = gg_parts(gg, n)
    w_ins, w_scratch = shared_parts(*weights)

    def body(r):
        t = Torus(n)
        shared = Shared(r)
        barrier_all(n)
        back = Exchange(t, n, lambda i: r.gg.at[i], r.dg, (r.qs, r.qr, r.ql))
        back.start()
        u = Return(t, r, 'u', rows_of[0], capacity, False)
        o = Return(t, r, 'o', rows_of[1], capacity, True)

        def work():
            shared.ready()
            shared.backward(r.xdy[:d], r.xdy[d:], r.ds)

        drive([o, u], work)
        r.last[...] = (r.x1dy[:d].astype(F32) + r.s[...] + o.out[...]).astype(BF16)
        r.dx[...] = (r.xdy[d:].astype(F32) + r.ds[...] + u.out[...]).astype(BF16)
        back.finish()

    res = run_kernel(body, cid, {**u_ins, **o_ins, **g_ins, **w_ins, 'lines': (lines, VMEM),
                                 'xdy': (block, VMEM), 'x1dy': (x1dy, VMEM), 's': (s, VMEM)},
                     {**g_outs, 'dx': ((d, tokens), BF16, VMEM), 'last': ((d, tokens), BF16, VMEM)},
                     {**u_scratch, **o_scratch, **g_scratch, **w_scratch, 'ds': VMEM((d, tokens), F32)})
    return res.dx, res.last, res.dg


def swiglu_grads(pre_gate, pre_up, d_hidden):
    sigma = jax.nn.sigmoid(pre_gate)
    d_gate = d_hidden * pre_up * sigma * (1.0 + pre_gate * (1.0 - sigma))
    d_up = d_hidden * pre_gate * sigma
    return d_gate.astype(BF16), d_up.astype(BF16)


def gate_table(idx, gate, n_experts):
    ids = jnp.arange(n_experts, dtype=idx.dtype)[:, None, None]
    return jnp.sum(jnp.where(idx.T[None] == ids, gate.T[None], 0.0), axis=1)


def pair_gates(dg, idx):
    ids = jnp.arange(dg.shape[0], dtype=idx.dtype)[:, None, None]
    return jnp.sum(jnp.where(idx.T[None] == ids, dg[:, None, :], 0.0), axis=0).T


def solution(mesh):
    n = mesh.shape['ep']
    token_spec = P(('dp', 'ep'), None)
    expert_spec = P('ep', None, None)
    shared_spec = P(None, None)
    grad_spec = P(('dp', 'ep'), None, None)
    layer_specs = (expert_spec,) * 3 + (shared_spec,) * 3

    def device_step(x_in, d_out, idx_a, gate_a, idx_b, gate_b,
                    w1_a, w3_a, w2_a, ws1_a, ws3_a, ws2_a,
                    w1_b, w3_b, w2_b, ws1_b, ws3_b, ws2_b):
        tokens, top_k = idx_a.shape
        n_experts = w1_a.shape[0] * n
        capacity = top_k * ((2 * tokens + n_experts - 1) // n_experts)

        flip = lambda w: jnp.swapaxes(w, 1, 2)
        w1_a, w3_a, w1_b, w3_b = flip(w1_a), flip(w3_a), flip(w1_b), flip(w3_b)

        odd = lax.rem(lax.axis_index('ep'), 2) == 1
        tables = [gate_table(i, g, n_experts).reshape(n, 2, tokens) for i, g in ((idx_a, gate_a), (idx_b, gate_b))]
        tables = [jnp.where(odd, t[:, ::-1], t) for t in tables]
        g_own = jnp.concatenate(tables + [jnp.zeros((n, 4, tokens), F32)], axis=1)

        x_t, dy_t = x_in.T, d_out.T
        shared_a, shared_b = (ws1_a, ws3_a, ws2_a), (ws1_b, ws3_b, ws2_b)
        xg, g_recv, lines = gather_first(x_t, g_own, n, 0)
        o_a = experts_forward(xg, g_recv, w1_a, w3_a, w2_a, 0, capacity)
        x1dy = return_first(o_a, lines, x_t, dy_t, shared_a, 0, capacity, n, 1)

        both = gather_block(x1dy, n, 2)
        experts_b = (w1_b, w3_b, w2_b)
        dw1_b, dw3_b, dw2_b, du_b, gg_b, rows_b = experts_backward(both, g_recv, *experts_b, 2, capacity, True)
        block, dg_b, o_b, s_b = return_second(du_b, gg_b, lines, x1dy, x_t, rows_b, experts_b, shared_b, 2, capacity, n, 3)

        both = gather_block(block, n, 4)
        dw1_a, dw3_a, dw2_a, du_a, gg_a = experts_backward(both, g_recv, w1_a, w3_a, w2_a, 0, capacity, False)
        d_first, x_last, dg_a = return_third(du_a, o_b, gg_a, lines, block, x1dy, s_b, shared_a, (0, 2), capacity, n, 5)
        x_last, d_first = x_last.T, d_first.T

        return (x_last, d_first, flip(dw1_a), flip(dw3_a), dw2_a, flip(dw1_b), flip(dw3_b), dw2_b,
                pair_gates(dg_a.reshape(n_experts, tokens), idx_a), pair_gates(dg_b.reshape(n_experts, tokens), idx_b))

    in_specs = (token_spec,) * 6 + layer_specs + layer_specs
    out_specs = (token_spec, token_spec) + (grad_spec,) * 6 + (token_spec, token_spec)
    return jax.shard_map(device_step, mesh=mesh, in_specs=in_specs, out_specs=out_specs, check_vma=False)
```
